32 devices in a mesh: row: 8 (over y, x, core), col: 4 (over z).
Axes of the slice: x: 2, y: 2, z: 4, core: 2. Of those that a mesh axis runs over, the one named last changes fastest.
Arguments:
- velocity: float32 [128, 128, 2048], P(None, 'row', 'col'), may hold values from -6 to 6
- symbol_x: float32 [128], replicated, may hold values from 0.3 to 3
- symbol_y: float32 [128], replicated, may hold values from 0.3 to 3
- symbol_z: float32 [2048], replicated, may hold values from 0.3 to 3
Outputs:
- coefficients: float32 [128, 128, 2048], P('row', 'col')
The draws below stay inside these ranges and needn't reach their ends.
All inputs are finite; a program needn't handle non-finite values.
Results may differ from the reference program's by a relative error of at most 0.000076.
Values sent between devices are 32-bit elements; how exact they have to be, the bound alone decides.
A program may use at most 192 MiB of HBM per device.

```python
import jax
import jax.numpy as jnp
from jax import lax

GRID_X = 128
GRID_Y = 128
GRID_Z = 2048


def level_of(own_key, shape, pieces, low, largest):
    factor_of = 1.0
    for dim, shards_of in pieces:
        draws = jax.random.uniform(jax.random.fold_in(jax.random.fold_in(own_key, 6), dim), (shards_of,), jnp.float32, low / len(pieces), largest / len(pieces))
        factor_of = factor_of * jnp.repeat(jnp.exp(draws), shape[dim] // shards_of).reshape((-1,) + (1,) * (len(shape) - 1 - dim))
    return factor_of


def normal_values(stream_key, dims, width, limit, split=(), held_as=jnp.bfloat16):
    drawn = jax.random.normal(stream_key, dims, jnp.float32) * width
    if len(split) > 0:
        drawn = level_of(stream_key, dims, split, -0.22, 0.18) * drawn
    return jnp.clip(drawn, min=-limit, max=limit).astype(held_as)


def setup_inputs(seed: int = 0) -> dict:
    seeds = jax.random.split(jax.random.key(seed), 5)
    velocity = normal_values(seeds[0], (GRID_X, GRID_Y, GRID_Z), 1.0, 6.0, ((1, 8), (2, 4)), jnp.float32)
    symbol_x = jnp.clip(jax.random.uniform(seeds[1], (GRID_X,), jnp.float32, 0.3, 3.0), 0.3, 3.0)
    symbol_y = jnp.clip(jax.random.uniform(seeds[2], (GRID_Y,), jnp.float32, 0.3, 3.0), 0.3, 3.0)
    symbol_z = jnp.clip(jax.random.uniform(seeds[3], (GRID_Z,), jnp.float32, 0.3, 3.0), 0.3, 3.0)
    return {"velocity": velocity, "symbol_x": symbol_x, "symbol_y": symbol_y, "symbol_z": symbol_z}


def mode_table(count):
    rank = jnp.arange(count)
    angle = (2.0 * jnp.pi / count) * ((rank[:, None] * rank[None, :]) % count).astype(jnp.float32)
    return (jnp.cos(angle) + jnp.sin(angle)) * (count ** -0.5)


def along_dim(values, dim):
    moved = jnp.tensordot(values, mode_table(values.shape[dim]), axes=([dim], [0]), precision=lax.Precision.HIGHEST)
    return jnp.moveaxis(moved, -1, dim)


def reference(velocity, symbol_x, symbol_y, symbol_z):
    coefficients = velocity
    coefficients = along_dim(coefficients, 0)
    coefficients = along_dim(coefficients, 1)
    coefficients = along_dim(coefficients, 2)
    symbol = symbol_x[:, None, None] + symbol_y[None, :, None] + symbol_z[None, None, :]
    coefficients = coefficients * ((1.0 - 0.2 * symbol) / (1.0 + 0.2 * symbol))
    return coefficients
```

```python
import functools

import jax
import jax.numpy as jnp
import numpy as np
from jax import lax
from jax.experimental import pallas as pl
from jax.experimental.pallas import tpu as pltpu
from jax.sharding import PartitionSpec as P

SUB = 8
MESH = pl.DeviceIdType.MESH


def mode_table(count):
    rank = jnp.arange(count)
    angle = 2.0 * jnp.pi / count * (rank[:, None] * rank[None, :] % count).astype(jnp.float32)
    return (jnp.cos(angle) + jnp.sin(angle)) * count ** (-0.5)


def along_dim(values, dim):
    moved = jnp.tensordot(
        values, mode_table(values.shape[dim]), axes=([dim], [0]), precision=lax.Precision.HIGHEST
    )
    return jnp.moveaxis(moved, -1, dim)


def fixed_table(count):
    rank = np.arange(count)
    angle = 2.0 * np.pi / count * (rank[:, None] * rank[None, :] % count)
    return ((np.cos(angle) + np.sin(angle)) * count ** (-0.5)).astype(np.float32)


def halves(table):
    high = table.astype(jnp.bfloat16)
    low = (table - high.astype(np.float32)).astype(jnp.bfloat16)
    return high, low


def split(values):
    high = values.astype(jnp.bfloat16)
    low = (values - high.astype(jnp.float32)).astype(jnp.bfloat16)
    return high, low


def product(a, b):
    return jnp.dot(a, b, preferred_element_type=jnp.float32)


def flipped(index, mask):
    out = index
    bit = 1
    while bit <= mask:
        if mask & bit:
            out = out + bit * (1 - 2 * ((index // bit) % 2))
        bit *= 2
    return out


def kernel(
    dims, v_hbm, w_hbm, t_hbm, sx_hbm, sy_hbm, sz_hbm, out_ref,
    v, w, t, v_parts, xs, rbuf, ybuf, zbuf, lhs, factors, sx_row, sy_row, sz_ref, sx_col, sy_col,
    load_sem, v_sem, row_send, row_recv, first_recv, col_send, col_recv, last_recv,
):
    rows, cols, chunks, per, lag, lanes = dims
    part_y, part_z = v.shape[1], v.shape[2]
    grid_x, grid_y = v.shape[0], rbuf.shape[1]
    share_y, grid_z = zbuf.shape[1], zbuf.shape[2]
    tiles, tile = t.shape[1], t.shape[3]
    r, c = lax.axis_index("row"), lax.axis_index("col")
    spans = [pl.ds(p * lanes, lanes) for p in range(part_z // lanes)]

    load_w = pltpu.make_async_copy(w_hbm.at[0], w.at[0], load_sem.at[1])
    load_rest = pltpu.make_async_copy(w_hbm.at[pl.ds(1, chunks - 1)], w.at[pl.ds(1, chunks - 1)], load_sem.at[2])
    load_t = pltpu.make_async_copy(t_hbm, t, load_sem.at[0])
    load_v = [
        pltpu.make_async_copy(v_hbm.at[:, :, span], v.at[:, :, span], v_sem.at[p])
        for p, span in enumerate(spans)
    ]
    load_symbols = [
        pltpu.make_async_copy(source, target, load_sem.at[3 + n])
        for n, (source, target) in enumerate(((sx_hbm, sx_row), (sy_hbm, sy_row), (sz_hbm, sz_ref)))
    ]
    half = cols // 2
    side = c // half
    row_masks = sorted(range(1, rows), key=lambda m: (-bin(m // 2).count("1"), m))
    row_peers = [flipped(r, m) for m in row_masks]
    near = [flipped(c, m) for m in range(1, half)]
    across = [(half + j) * (1 - side) + (half - 1 - j) * side for j in range(half)]
    col_peers = near + across
    depth = (half - 1 - c) * (1 - side) + (c - half) * side
    col_marks = list(range(half - 1)) + [half - 1 + depth] * half

    barrier = pltpu.get_barrier_semaphore()
    for s in row_peers:
        pl.semaphore_signal(barrier, inc=1, device_id=(s, c), device_id_type=MESH)
    for s in col_peers:
        pl.semaphore_signal(barrier, inc=1, device_id=(r, s), device_id_type=MESH)
    load_w.start()
    for load in load_v + load_symbols:
        load.start()

    step = SUB * SUB
    whole = pl.ds(0, part_z)
    piece = part_z // 2 if part_z % 256 == 0 else part_z
    ends = [pl.ds(q * piece, piece) for q in range(part_z // piece)]

    def split_parts(span):
        def part_loop(i, carry):
            for g in range(part_y // SUB):
                block = v[pl.ds(i * SUB, SUB), g * SUB:(g + 1) * SUB, span].reshape(step, lanes)
                high, low = split(block)
                v_parts[g, 0, pl.ds(pl.multiple_of(i * step, step), step), span] = high
                v_parts[g, 1, pl.ds(pl.multiple_of(i * step, step), step), span] = low
            return carry

        lax.fori_loop(0, grid_x // SUB, part_loop, 0)

    def x_stage(k, span):
        m, depth = rows * per * SUB, grid_x * SUB
        for g in range(part_y // SUB):
            both = product(w[k, :2 * m, :depth], v_parts[g, 0, :, span])
            sums = both[:m] + both[m:] + product(w[k, :m, :depth], v_parts[g, 1, :, span])
            xs[k, :, g * SUB:(g + 1) * SUB, span] = sums.reshape(rows * per, SUB, span.size)

    def own_rows():
        return pl.ds(pl.multiple_of(r * part_y, SUB), part_y)

    def row_stage(k, span, recv):
        for i in range(per):
            for s in row_peers:
                pltpu.make_async_remote_copy(
                    src_ref=xs.at[k, s * per + i, :, span],
                    dst_ref=rbuf.at[k * per + i, own_rows(), span],
                    send_sem=row_send.at[k], recv_sem=recv.at[i],
                    device_id=(s, c), device_id_type=MESH,
                ).start()
        rbuf[pl.ds(k * per, per), own_rows(), span] = xs[k, pl.ds(r * per, per), :, span]

    def y_plane(k, i, span, recv):
        came = rbuf.at[k * per + i, pl.ds(0, grid_y - part_y), span]
        pltpu.make_async_copy(came, came, recv.at[i]).wait()
        high, low = split(rbuf[k * per + i, :, span])
        both = product(w[0, :2 * grid_y, grid_x * SUB:], high)
        ybuf[k, i, :, span] = both[:grid_y] + both[grid_y:] + product(w[0, :grid_y, grid_x * SUB:], low)

    def col_stage(k, i, span, recv):
        at = pl.ds(pl.multiple_of(c * part_z + span.start, 128), span.size)
        for s, mark in zip(col_peers, col_marks):
            pltpu.make_async_remote_copy(
                src_ref=ybuf.at[k, i, pl.ds(pl.multiple_of(s * share_y, SUB), share_y), span],
                dst_ref=zbuf.at[k * per + i, :, at],
                send_sem=col_send.at[k], recv_sem=recv.at[mark],
                device_id=(r, s), device_id_type=MESH,
            ).start()

    def y_stage(k, span, recv):
        for i in range(per):
            y_plane(k, i, span, recv)
            col_stage(k, i, span, col_recv.at[k])

    def last_y_stage(k, recv):
        for i in range(per):
            y_plane(k, i, whole, recv)
        for q, span in enumerate(ends):
            for i in range(per):
                col_stage(k, i, span, last_recv.at[q])

    def own_z(k):
        zbuf[pl.ds(k * per, per), :, pl.ds(pl.multiple_of(c * part_z, 128), part_z)] = (
            ybuf[k, :, pl.ds(pl.multiple_of(c * share_y, SUB), share_y), :]
        )

    def col_wait(k, m):
        came = zbuf.at[pl.ds(k * per, per), :, pl.ds(0, part_z)]
        pltpu.make_async_copy(came, came, col_recv.at[k, m]).wait()

    def factor_parts(k, n):
        y_part = sy_col[pl.ds(pl.multiple_of(c * share_y, SUB), share_y), :]
        z_part = sz_ref[:, pl.ds(pl.multiple_of(n * tile, tile), tile)]
        plane = jnp.concatenate([y_part] * (tile // 128), axis=1) + z_part
        for i in range(per):
            x_part = sx_col[pl.ds(r * chunks * per + k * per + i, 1), :]
            symbol = jnp.concatenate([x_part] * (tile // 128), axis=1) + plane
            yield i, (1.0 - 0.2 * symbol) / (1.0 + 0.2 * symbol)

    size = per * share_y

    def scaled(k, n, sums):
        for i, factor in factor_parts(k, n):
            out_ref[k * per + i, :, pl.ds(pl.multiple_of(n * tile, tile), tile)] = (
                sums[i * share_y:(i + 1) * share_y] * factor
            )

    def z_stage(k):
        for m in range(len(col_peers)):
            col_wait(k, m)
        high, low = split(zbuf[pl.ds(k * per, per)].reshape(size, grid_z))
        lhs[:size] = high
        lhs[size:] = low

        def tile_loop(n, carry):
            both = product(lhs[...], t[0, n])
            scaled(k, n, both[:size] + both[size:] + product(lhs[:size], t[1, n]))
            return carry

        lax.fori_loop(0, tiles, tile_loop, 0, unroll=2)

    def z_part(k, start, count, finish=None):
        span = pl.ds(pl.multiple_of(start, 128), count)
        high, low = split(zbuf[pl.ds(k * per, per), :, span].reshape(size, count))
        lhs[:size, :count] = high
        lhs[size:, :count] = low

        def tile_loop(n, carry):
            both = product(lhs[:, :count], t[0, n, span, :])
            sums = both[:size] + both[size:] + product(lhs[:size, :count], t[1, n, span, :])
            at = pl.ds(pl.multiple_of(n * tile, tile), tile)
            if count < grid_z // 2:
                sums = sums + out_ref[pl.ds(k * per, per), :, at].reshape(size, tile)
            if finish is None:
                out_ref[pl.ds(k * per, per), :, at] = sums.reshape(per, share_y, tile)
            else:
                finish(k, n, sums)
            return carry

        lax.fori_loop(0, tiles, tile_loop, 0, unroll=4)

    def prepare(k):
        def tile_loop(n, carry):
            for i, factor in factor_parts(k, n):
                factors[i, :, pl.ds(pl.multiple_of(n * tile, tile), tile)] = factor
            return carry

        lax.fori_loop(0, tiles, tile_loop, 0)

    def multiplied(k, n, sums):
        at = pl.ds(pl.multiple_of(n * tile, tile), tile)
        out_ref[pl.ds(k * per, per), :, at] = sums.reshape(per, share_y, tile) * factors[:, :, at]

    def last_wait(q, m):
        came = zbuf.at[pl.ds((chunks - 1) * per, per), :, pl.ds(0, piece)]
        pltpu.make_async_copy(came, came, last_recv.at[q, m]).wait()

    def last_z_stages():
        before, last = chunks - 2, chunks - 1
        for m in range(len(near)):
            col_wait(before, m)
        z_part(before, side * half * part_z, half * part_z)
        for j in range(half - 1):
            col_wait(before, len(near) + j)
            z_part(before, across[j] * part_z, part_z)
        for m in range(len(near)):
            for q in range(len(ends)):
                last_wait(q, m)
        z_part(last, side * half * part_z, half * part_z)
        prepare(last)
        for j in range(half - 1):
            for q in range(len(ends)):
                last_wait(q, len(near) + j)
            z_part(last, across[j] * part_z, part_z)
        col_wait(before, len(col_peers) - 1)
        z_part(before, across[-1] * part_z, part_z, scaled)
        for q, span in enumerate(ends):
            last_wait(q, len(col_peers) - 1)
            z_part(last, across[-1] * part_z + span.start, piece, multiplied if q == len(ends) - 1 else None)

    for p, span in enumerate(spans):
        load_v[p].wait()
        split_parts(span)
        if p == 0:
            load_w.wait()
        x_stage(0, span)
        if p == 0:
            pl.semaphore_wait(barrier, len(row_peers) + len(col_peers))
        row_stage(0, span, first_recv.at[p])
    load_rest.start()
    load_t.start()
    y_stage(0, spans[0], first_recv.at[0])
    load_rest.wait()
    x_stage(1, whole)
    row_stage(1, whole, row_recv.at[1])
    for p, span in enumerate(spans[1:]):
        y_stage(0, span, first_recv.at[p + 1])
    own_z(0)
    for load in load_symbols:
        load.wait()
    for ref, column in ((sx_row, sx_col), (sy_row, sy_col)):
        column[...] = jnp.broadcast_to(ref[...], (128, ref.shape[1])).T

    def loop(k, carry):
        @pl.when(k < chunks)
        def _():
            x_stage(k, whole)
            row_stage(k, whole, row_recv.at[k])

        @pl.when(k < chunks)
        def _():
            y_stage(k - 1, whole, row_recv.at[k - 1])
            own_z(k - 1)

        @pl.when(k == chunks)
        def _():
            last_y_stage(chunks - 1, row_recv.at[chunks - 1])
            own_z(chunks - 1)

        @pl.when(k == lag + 1)
        def _():
            load_t.wait()

        @pl.when(k >= lag + 1)
        def _():
            z_stage(k - 1 - lag)

        return carry

    lax.fori_loop(2, chunks + lag - 1, loop, 0)
    last_z_stages()

    def drain(k, carry):
        sent = rbuf.at[pl.ds(k * per, per), pl.ds(0, grid_y - part_y), :]
        pltpu.make_async_copy(sent, sent, row_send.at[k]).wait()
        sent = zbuf.at[pl.ds(k * per, per), :, pl.ds(0, grid_z - part_z)]
        pltpu.make_async_copy(sent, sent, col_send.at[k]).wait()
        return carry

    lax.fori_loop(0, chunks, drain, 0)


def transformed(rows, cols, velocity, symbol_x, symbol_y, symbol_z):
    grid_x, part_y, part_z = velocity.shape
    grid_y, grid_z = part_y * rows, part_z * cols
    share_x, share_y = grid_x // rows, grid_y // cols
    chunks = min(8, share_x)
    per = share_x // chunks
    tile = 256
    hx, hy, hz = fixed_table(grid_x), fixed_table(grid_y), fixed_table(grid_z)
    order = np.arange(grid_x).reshape(rows, chunks, per).transpose(1, 0, 2).reshape(chunks, rows * per)
    w = np.stack([np.kron(hx[o], np.eye(SUB, dtype=np.float32)) for o in order])
    w = np.concatenate(halves(w), axis=1)
    h = np.concatenate(halves(hy), axis=0)
    t = np.stack(halves(hz)).reshape(2, grid_z, grid_z // tile, tile).transpose(0, 2, 1, 3)
    held = np.zeros((chunks, max(w.shape[1], h.shape[0]), w.shape[2] + h.shape[1]), w.dtype)
    held[:, :w.shape[1], :w.shape[2]] = w
    held[0, :h.shape[0], w.shape[2]:] = h
    f32, bf16 = jnp.float32, jnp.bfloat16
    hbm = pl.BlockSpec(memory_space=pltpu.HBM)
    vmem = pl.BlockSpec(memory_space=pltpu.VMEM)
    return pl.pallas_call(
        functools.partial(kernel, (rows, cols, chunks, per, 2, 128)),
        out_shape=jax.ShapeDtypeStruct((share_x, share_y, grid_z), f32),
        in_specs=[hbm] * 6,
        out_specs=vmem,
        scratch_shapes=[
            pltpu.VMEM(velocity.shape, f32),
            pltpu.VMEM(held.shape, bf16),
            pltpu.VMEM(t.shape, bf16),
            pltpu.VMEM((part_y // SUB, 2, grid_x * SUB, part_z), bf16),
            pltpu.VMEM((chunks, rows * per, part_y, part_z), f32),
            pltpu.VMEM((share_x, grid_y, part_z), f32),
            pltpu.VMEM((chunks, per, grid_y, part_z), f32),
            pltpu.VMEM((share_x, share_y, grid_z), f32),
            pltpu.VMEM((2 * per * share_y, grid_z), bf16),
            pltpu.VMEM((per, share_y, grid_z), f32),
            pltpu.VMEM((1, grid_x), f32),
            pltpu.VMEM((1, grid_y), f32),
            pltpu.VMEM((1, grid_z), f32),
            pltpu.VMEM((grid_x, 128), f32),
            pltpu.VMEM((grid_y, 128), f32),
            pltpu.SemaphoreType.DMA((6,)),
            pltpu.SemaphoreType.DMA((part_z // 128,)),
            pltpu.SemaphoreType.DMA((chunks,)),
            pltpu.SemaphoreType.DMA((chunks, per)),
            pltpu.SemaphoreType.DMA((part_z // 128, per)),
            pltpu.SemaphoreType.DMA((chunks,)),
            pltpu.SemaphoreType.DMA((chunks, cols - 1)),
            pltpu.SemaphoreType.DMA((2, cols - 1)),
        ],
        compiler_params=pltpu.CompilerParams(
            collective_id=0, has_side_effects=True, vmem_limit_bytes=47 * 2**20
        ),
    )(velocity, jnp.asarray(held), jnp.asarray(np.ascontiguousarray(t)),
      *(pltpu.with_memory_space_constraint(symbol[None, :], pltpu.HBM) for symbol in (symbol_x, symbol_y, symbol_z)))


def fits(rows, cols, shape):
    grid_x, part_y, part_z = shape
    grid_z = part_z * cols
    held = 7 * grid_x * part_y * part_z * 4 + 4 * grid_z * grid_z + 4 * (grid_x * SUB) ** 2
    even = rows & (rows - 1) == 0 and cols & (cols - 1) == 0 and cols > 1 and grid_x % (8 * rows) == 0
    return even and part_y % SUB == 0 and part_z % 128 == 0 and (part_y * rows) % (SUB * cols) == 0 and held < 54 * 2**20


def local(rows, cols, velocity, symbol_x, symbol_y, symbol_z):
    if fits(rows, cols, velocity.shape):
        return transformed(rows, cols, velocity, symbol_x, symbol_y, symbol_z)
    part_values = along_dim(velocity, 0)
    part_values = lax.all_to_all(part_values, "row", split_axis=0, concat_axis=1, tiled=True)
    pencil_values = along_dim(part_values, 1)
    pencil_values = lax.all_to_all(pencil_values, "col", split_axis=1, concat_axis=2, tiled=True)
    pencil_values = along_dim(pencil_values, 2)
    share_x = pencil_values.shape[0]
    part_x = lax.dynamic_slice_in_dim(symbol_x, lax.axis_index("row") * share_x, share_x)
    share_y = pencil_values.shape[1]
    part_y = lax.dynamic_slice_in_dim(symbol_y, lax.axis_index("col") * share_y, share_y)
    symbol = part_x[:, None, None] + part_y[None, :, None] + symbol_z[None, None, :]
    return pencil_values * ((1.0 - 0.2 * symbol) / (1.0 + 0.2 * symbol))


def solution(mesh):
    placed = (P(None, "row", "col"), P(), P(), P())
    return jax.shard_map(
        functools.partial(local, mesh.shape["row"], mesh.shape["col"]),
        mesh=mesh, in_specs=placed, out_specs=P("row", "col", None), check_vma=False,
    )
```

```python
import functools

import jax
import jax.numpy as jnp
import numpy as np
from jax import lax
from jax.experimental import pallas as pl
from jax.experimental.pallas import tpu as pltpu
from jax.sharding import PartitionSpec as P

SUB = 8
MESH = pl.DeviceIdType.MESH


def mode_table(count):
    rank = jnp.arange(count)
    angle = 2.0 * jnp.pi / count * (rank[:, None] * rank[None, :] % count).astype(jnp.float32)
    return (jnp.cos(angle) + jnp.sin(angle)) * count ** (-0.5)


def along_dim(values, dim):
    moved = jnp.tensordot(
        values, mode_table(values.shape[dim]), axes=([dim], [0]), precision=lax.Precision.HIGHEST
    )
    return jnp.moveaxis(moved, -1, dim)


def fixed_table(count):
    rank = np.arange(count)
    angle = 2.0 * np.pi / count * (rank[:, None] * rank[None, :] % count)
    return ((np.cos(angle) + np.sin(angle)) * count ** (-0.5)).astype(np.float32)


def halves(table):
    high = table.astype(jnp.bfloat16)
    low = (table - high.astype(np.float32)).astype(jnp.bfloat16)
    return high, low


def split(values):
    high = values.astype(jnp.bfloat16)
    low = (values - high.astype(jnp.float32)).astype(jnp.bfloat16)
    return high, low


def product(a, b):
    return jnp.dot(a, b, preferred_element_type=jnp.float32)


def flipped(index, mask):
    out = index
    bit = 1
    while bit <= mask:
        if mask & bit:
            out = out + bit * (1 - 2 * ((index // bit) % 2))
        bit *= 2
    return out


def kernel(
    dims, v_hbm, w_hbm, t_hbm, sx_hbm, sy_hbm, sz_hbm, out_ref,
    v, w, t, v_parts, xs, rbuf, ybuf, zbuf, lhs, factors, sx_row, sy_row, sz_ref, sx_col, sy_col,
    load_sem, v_sem, row_send, row_recv, first_recv, col_send, col_recv, last_recv,
):
    rows, cols, chunks, per, lag, lanes = dims
    part_y, part_z = v.shape[1], v.shape[2]
    grid_x, grid_y = v.shape[0], rbuf.shape[1]
    share_y, grid_z = zbuf.shape[1], zbuf.shape[2]
    tiles, tile = t.shape[1], t.shape[3]
    r, c = lax.axis_index("row"), lax.axis_index("col")
    spans = [pl.ds(p * lanes, lanes) for p in range(part_z // lanes)]

    load_w = pltpu.make_async_copy(w_hbm.at[0], w.at[0], load_sem.at[1])
    load_rest = pltpu.make_async_copy(w_hbm.at[pl.ds(1, chunks - 1)], w.at[pl.ds(1, chunks - 1)], load_sem.at[2])
    load_t = pltpu.make_async_copy(t_hbm, t, load_sem.at[0])
    load_v = [
        pltpu.make_async_copy(v_hbm.at[:, :, span], v.at[:, :, span], v_sem.at[p])
        for p, span in enumerate(spans)
    ]
    load_symbols = [
        pltpu.make_async_copy(source, target, load_sem.at[3 + n])
        for n, (source, target) in enumerate(((sx_hbm, sx_row), (sy_hbm, sy_row), (sz_hbm, sz_ref)))
    ]
    half = cols // 2
    side = c // half
    row_masks = sorted(range(1, rows), key=lambda m: (-bin(m // 2).count("1"), m))
    row_peers = [flipped(r, m) for m in row_masks]
    near = [flipped(c, m) for m in range(1, half)]
    across = [(half + j) * (1 - side) + (half - 1 - j) * side for j in reversed(range(half))]
    col_peers = near + across
    depth = (half - 1 - c) * (1 - side) + (c - half) * side
    marks = list(range(half - 1)) + [2 * half - 2 - depth] * half
    col_targets = list(zip(col_peers, marks))

    barrier = pltpu.get_barrier_semaphore()
    for s in row_peers:
        pl.semaphore_signal(barrier, inc=1, device_id=(s, c), device_id_type=MESH)
    for s in col_peers:
        pl.semaphore_signal(barrier, inc=1, device_id=(r, s), device_id_type=MESH)
    load_w.start()
    for load in load_v + load_symbols:
        load.start()

    step = SUB * SUB
    whole = pl.ds(0, part_z)
    piece = part_z // 2 if part_z % 256 == 0 else part_z
    ends = [pl.ds(q * piece, piece) for q in range(part_z // piece)]

    def split_parts(span):
        def part_loop(i, carry):
            for g in range(part_y // SUB):
                block = v[pl.ds(i * SUB, SUB), g * SUB:(g + 1) * SUB, span].reshape(step, lanes)
                high, low = split(block)
                v_parts[g, 0, pl.ds(pl.multiple_of(i * step, step), step), span] = high
                v_parts[g, 1, pl.ds(pl.multiple_of(i * step, step), step), span] = low
            return carry

        lax.fori_loop(0, grid_x // SUB, part_loop, 0)

    def x_stage(k, span):
        m, depth = rows * per * SUB, grid_x * SUB
        for g in range(part_y // SUB):
            both = product(w[k, :2 * m, :depth], v_parts[g, 0, :, span])
            sums = both[:m] + both[m:] + product(w[k, :m, :depth], v_parts[g, 1, :, span])
            xs[k, :, g * SUB:(g + 1) * SUB, span] = sums.reshape(rows * per, SUB, span.size)

    def own_rows():
        return pl.ds(pl.multiple_of(r * part_y, SUB), part_y)

    def row_stage(k, span, recv):
        for i in range(per):
            for s in row_peers:
                pltpu.make_async_remote_copy(
                    src_ref=xs.at[k, s * per + i, :, span],
                    dst_ref=rbuf.at[k * per + i, own_rows(), span],
                    send_sem=row_send.at[k], recv_sem=recv.at[i],
                    device_id=(s, c), device_id_type=MESH,
                ).start()
        rbuf[pl.ds(k * per, per), own_rows(), span] = xs[k, pl.ds(r * per, per), :, span]

    def y_plane(k, i, span, recv):
        came = rbuf.at[k * per + i, pl.ds(0, grid_y - part_y), span]
        pltpu.make_async_copy(came, came, recv.at[i]).wait()
        high, low = split(rbuf[k * per + i, :, span])
        both = product(w[0, :2 * grid_y, grid_x * SUB:], high)
        ybuf[k, i, :, span] = both[:grid_y] + both[grid_y:] + product(w[0, :grid_y, grid_x * SUB:], low)

    def col_stage(k, i, span, recv, targets):
        at = pl.ds(pl.multiple_of(c * part_z + span.start, 128), span.size)
        for s, mark in targets:
            pltpu.make_async_remote_copy(
                src_ref=ybuf.at[k, i, pl.ds(pl.multiple_of(s * share_y, SUB), share_y), span],
                dst_ref=zbuf.at[k * per + i, :, at],
                send_sem=col_send.at[k], recv_sem=recv.at[mark],
                device_id=(r, s), device_id_type=MESH,
            ).start()

    def y_stage(k, span, recv):
        for i in range(per):
            y_plane(k, i, span, recv)
            col_stage(k, i, span, col_recv.at[k], col_targets)

    def last_y_stage(k, recv):
        for i in range(per):
            y_plane(k, i, whole, recv)
        for target in col_targets:
            for q, span in enumerate(ends):
                for i in range(per):
                    col_stage(k, i, span, last_recv.at[q], [target])

    def own_z(k):
        zbuf[pl.ds(k * per, per), :, pl.ds(pl.multiple_of(c * part_z, 128), part_z)] = (
            ybuf[k, :, pl.ds(pl.multiple_of(c * share_y, SUB), share_y), :]
        )

    def col_wait(k, m):
        came = zbuf.at[pl.ds(k * per, per), :, pl.ds(0, part_z)]
        pltpu.make_async_copy(came, came, col_recv.at[k, m]).wait()

    def factor_parts(k, n):
        y_part = sy_col[pl.ds(pl.multiple_of(c * share_y, SUB), share_y), :]
        z_part = sz_ref[:, pl.ds(pl.multiple_of(n * tile, tile), tile)]
        plane = jnp.concatenate([y_part] * (tile // 128), axis=1) + z_part
        for i in range(per):
            x_part = sx_col[pl.ds(r * chunks * per + k * per + i, 1), :]
            symbol = jnp.concatenate([x_part] * (tile // 128), axis=1) + plane
            yield i, (1.0 - 0.2 * symbol) / (1.0 + 0.2 * symbol)

    size = per * share_y

    def scaled(k, n, sums):
        for i, factor in factor_parts(k, n):
            out_ref[k * per + i, :, pl.ds(pl.multiple_of(n * tile, tile), tile)] = (
                sums[i * share_y:(i + 1) * share_y] * factor
            )

    def z_stage(k):
        for m in range(len(col_peers)):
            col_wait(k, m)
        high, low = split(zbuf[pl.ds(k * per, per)].reshape(size, grid_z))
        lhs[:size] = high
        lhs[size:] = low

        def tile_loop(n, carry):
            both = product(lhs[...], t[0, n])
            scaled(k, n, both[:size] + both[size:] + product(lhs[:size], t[1, n]))
            return carry

        lax.fori_loop(0, tiles, tile_loop, 0, unroll=2)

    def z_part(k, start, count, finish=None):
        span = pl.ds(pl.multiple_of(start, 128), count)
        high, low = split(zbuf[pl.ds(k * per, per), :, span].reshape(size, count))
        lhs[:size, :count] = high
        lhs[size:, :count] = low

        def tile_loop(n, carry):
            both = product(lhs[:, :count], t[0, n, span, :])
            sums = both[:size] + both[size:] + product(lhs[:size, :count], t[1, n, span, :])
            at = pl.ds(pl.multiple_of(n * tile, tile), tile)
            if count < grid_z // 2:
                sums = sums + out_ref[pl.ds(k * per, per), :, at].reshape(size, tile)
            if finish is None:
                out_ref[pl.ds(k * per, per), :, at] = sums.reshape(per, share_y, tile)
            else:
                finish(k, n, sums)
            return carry

        lax.fori_loop(0, tiles, tile_loop, 0, unroll=4)

    def prepare(k):
        def tile_loop(n, carry):
            for i, factor in factor_parts(k, n):
                factors[i, :, pl.ds(pl.multiple_of(n * tile, tile), tile)] = factor
            return carry

        lax.fori_loop(0, tiles, tile_loop, 0)

    def multiplied(k, n, sums):
        at = pl.ds(pl.multiple_of(n * tile, tile), tile)
        out_ref[pl.ds(k * per, per), :, at] = sums.reshape(per, share_y, tile) * factors[:, :, at]

    def last_wait(q, m):
        came = zbuf.at[pl.ds((chunks - 1) * per, per), :, pl.ds(0, piece)]
        pltpu.make_async_copy(came, came, last_recv.at[q, m]).wait()

    def last_z_stages():
        before, last = chunks - 2, chunks - 1
        for m in range(len(near)):
            col_wait(before, m)
        z_part(before, side * half * part_z, half * part_z)
        for j in range(half - 1):
            col_wait(before, len(near) + j)
            z_part(before, across[j] * part_z, part_z)
        for m in range(len(near)):
            for q in range(len(ends)):
                last_wait(q, m)
        z_part(last, side * half * part_z, half * part_z)
        prepare(last)
        for j in range(half - 1):
            for q in range(len(ends)):
                last_wait(q, len(near) + j)
            z_part(last, across[j] * part_z, part_z)
        col_wait(before, len(col_peers) - 1)
        z_part(before, across[-1] * part_z, part_z, scaled)
        for q, span in enumerate(ends):
            last_wait(q, len(col_peers) - 1)
            z_part(last, across[-1] * part_z + span.start, piece, multiplied if q == len(ends) - 1 else None)

    for p, span in enumerate(spans):
        load_v[p].wait()
        split_parts(span)
        if p == 0:
            load_w.wait()
        x_stage(0, span)
        if p == 0:
            pl.semaphore_wait(barrier, len(row_peers) + len(col_peers))
        row_stage(0, span, first_recv.at[p])
    load_rest.start()
    load_t.start()
    y_stage(0, spans[0], first_recv.at[0])
    load_rest.wait()
    x_stage(1, whole)
    row_stage(1, whole, row_recv.at[1])
    for p, span in enumerate(spans[1:]):
        y_stage(0, span, first_recv.at[p + 1])
    own_z(0)
    for load in load_symbols:
        load.wait()
    for ref, column in ((sx_row, sx_col), (sy_row, sy_col)):
        column[...] = jnp.broadcast_to(ref[...], (128, ref.shape[1])).T

    def loop(k, carry):
        @pl.when(k < chunks)
        def _():
            x_stage(k, whole)
            row_stage(k, whole, row_recv.at[k])

        @pl.when(k < chunks)
        def _():
            y_stage(k - 1, whole, row_recv.at[k - 1])
            own_z(k - 1)

        @pl.when(k == chunks)
        def _():
            last_y_stage(chunks - 1, row_recv.at[chunks - 1])
            own_z(chunks - 1)

        @pl.when(k == lag + 1)
        def _():
            load_t.wait()

        @pl.when(k >= lag + 1)
        def _():
            z_stage(k - 1 - lag)

        return carry

    lax.fori_loop(2, chunks + lag - 1, loop, 0)
    last_z_stages()

    def drain(k, carry):
        sent = rbuf.at[pl.ds(k * per, per), pl.ds(0, grid_y - part_y), :]
        pltpu.make_async_copy(sent, sent, row_send.at[k]).wait()
        sent = zbuf.at[pl.ds(k * per, per), :, pl.ds(0, grid_z - part_z)]
        pltpu.make_async_copy(sent, sent, col_send.at[k]).wait()
        return carry

    lax.fori_loop(0, chunks, drain, 0)


def transformed(rows, cols, velocity, symbol_x, symbol_y, symbol_z):
    grid_x, part_y, part_z = velocity.shape
    grid_y, grid_z = part_y * rows, part_z * cols
    share_x, share_y = grid_x // rows, grid_y // cols
    chunks = min(8, share_x)
    per = share_x // chunks
    tile = 256
    hx, hy, hz = fixed_table(grid_x), fixed_table(grid_y), fixed_table(grid_z)
    order = np.arange(grid_x).reshape(rows, chunks, per).transpose(1, 0, 2).reshape(chunks, rows * per)
    w = np.stack([np.kron(hx[o], np.eye(SUB, dtype=np.float32)) for o in order])
    w = np.concatenate(halves(w), axis=1)
    h = np.concatenate(halves(hy), axis=0)
    t = np.stack(halves(hz)).reshape(2, grid_z, grid_z // tile, tile).transpose(0, 2, 1, 3)
    held = np.zeros((chunks, max(w.shape[1], h.shape[0]), w.shape[2] + h.shape[1]), w.dtype)
    held[:, :w.shape[1], :w.shape[2]] = w
    held[0, :h.shape[0], w.shape[2]:] = h
    f32, bf16 = jnp.float32, jnp.bfloat16
    hbm = pl.BlockSpec(memory_space=pltpu.HBM)
    vmem = pl.BlockSpec(memory_space=pltpu.VMEM)
    return pl.pallas_call(
        functools.partial(kernel, (rows, cols, chunks, per, 2, 128)),
        out_shape=jax.ShapeDtypeStruct((share_x, share_y, grid_z), f32),
        in_specs=[hbm] * 6,
        out_specs=vmem,
        scratch_shapes=[
            pltpu.VMEM(velocity.shape, f32),
            pltpu.VMEM(held.shape, bf16),
            pltpu.VMEM(t.shape, bf16),
            pltpu.VMEM((part_y // SUB, 2, grid_x * SUB, part_z), bf16),
            pltpu.VMEM((chunks, rows * per, part_y, part_z), f32),
            pltpu.VMEM((share_x, grid_y, part_z), f32),
            pltpu.VMEM((chunks, per, grid_y, part_z), f32),
            pltpu.VMEM((share_x, share_y, grid_z), f32),
            pltpu.VMEM((2 * per * share_y, grid_z), bf16),
            pltpu.VMEM((per, share_y, grid_z), f32),
            pltpu.VMEM((1, grid_x), f32),
            pltpu.VMEM((1, grid_y), f32),
            pltpu.VMEM((1, grid_z), f32),
            pltpu.VMEM((grid_x, 128), f32),
            pltpu.VMEM((grid_y, 128), f32),
            pltpu.SemaphoreType.DMA((6,)),
            pltpu.SemaphoreType.DMA((part_z // 128,)),
            pltpu.SemaphoreType.DMA((chunks,)),
            pltpu.SemaphoreType.DMA((chunks, per)),
            pltpu.SemaphoreType.DMA((part_z // 128, per)),
            pltpu.SemaphoreType.DMA((chunks,)),
            pltpu.SemaphoreType.DMA((chunks, cols - 1)),
            pltpu.SemaphoreType.DMA((2, cols - 1)),
        ],
        compiler_params=pltpu.CompilerParams(
            collective_id=0, has_side_effects=True, vmem_limit_bytes=47 * 2**20
        ),
    )(velocity, jnp.asarray(held), jnp.asarray(np.ascontiguousarray(t)),
      *(pltpu.with_memory_space_constraint(symbol[None, :], pltpu.HBM) for symbol in (symbol_x, symbol_y, symbol_z)))


def fits(rows, cols, shape):
    grid_x, part_y, part_z = shape
    grid_z = part_z * cols
    held = 7 * grid_x * part_y * part_z * 4 + 4 * grid_z * grid_z + 4 * (grid_x * SUB) ** 2
    even = rows & (rows - 1) == 0 and cols & (cols - 1) == 0 and cols > 1 and grid_x % (8 * rows) == 0
    return even and part_y % SUB == 0 and part_z % 128 == 0 and (part_y * rows) % (SUB * cols) == 0 and held < 54 * 2**20


def local(rows, cols, velocity, symbol_x, symbol_y, symbol_z):
    if fits(rows, cols, velocity.shape):
        return transformed(rows, cols, velocity, symbol_x, symbol_y, symbol_z)
    part_values = along_dim(velocity, 0)
    part_values = lax.all_to_all(part_values, "row", split_axis=0, concat_axis=1, tiled=True)
    pencil_values = along_dim(part_values, 1)
    pencil_values = lax.all_to_all(pencil_values, "col", split_axis=1, concat_axis=2, tiled=True)
    pencil_values = along_dim(pencil_values, 2)
    share_x = pencil_values.shape[0]
    part_x = lax.dynamic_slice_in_dim(symbol_x, lax.axis_index("row") * share_x, share_x)
    share_y = pencil_values.shape[1]
    part_y = lax.dynamic_slice_in_dim(symbol_y, lax.axis_index("col") * share_y, share_y)
    symbol = part_x[:, None, None] + part_y[None, :, None] + symbol_z[None, None, :]
    return pencil_values * ((1.0 - 0.2 * symbol) / (1.0 + 0.2 * symbol))


def solution(mesh):
    placed = (P(None, "row", "col"), P(), P(), P())
    return jax.shard_map(
        functools.partial(local, mesh.shape["row"], mesh.shape["col"]),
        mesh=mesh, in_specs=placed, out_specs=P("row", "col", None), check_vma=False,
    )
```

```python
import functools

import jax
import jax.numpy as jnp
import numpy as np
from jax import lax
from jax.experimental import pallas as pl
from jax.experimental.pallas import tpu as pltpu
from jax.sharding import PartitionSpec as P

SUB = 8
MESH = pl.DeviceIdType.MESH


def mode_table(count):
    rank = jnp.arange(count)
    angle = 2.0 * jnp.pi / count * (rank[:, None] * rank[None, :] % count).astype(jnp.float32)
    return (jnp.cos(angle) + jnp.sin(angle)) * count ** (-0.5)


def along_dim(values, dim):
    moved = jnp.tensordot(
        values, mode_table(values.shape[dim]), axes=([dim], [0]), precision=lax.Precision.HIGHEST
    )
    return jnp.moveaxis(moved, -1, dim)


def fixed_table(count):
    rank = np.arange(count)
    angle = 2.0 * np.pi / count * (rank[:, None] * rank[None, :] % count)
    return ((np.cos(angle) + np.sin(angle)) * count ** (-0.5)).astype(np.float32)


def halves(table):
    high = table.astype(jnp.bfloat16)
    low = (table - high.astype(np.float32)).astype(jnp.bfloat16)
    return high, low


def split(values):
    high = values.astype(jnp.bfloat16)
    low = (values - high.astype(jnp.float32)).astype(jnp.bfloat16)
    return high, low


def product(a, b):
    return jnp.dot(a, b, preferred_element_type=jnp.float32)


def flipped(index, mask):
    out = index
    bit = 1
    while bit <= mask:
        if mask & bit:
            out = out + bit * (1 - 2 * ((index // bit) % 2))
        bit *= 2
    return out


def kernel(
    dims, v_hbm, w_hbm, t_hbm, sx_hbm, sy_hbm, sz_hbm, out_ref,
    v, w, t, v_parts, xs, rbuf, ybuf, zbuf, lhs, factors, raw_in, raw_all, raw_y, sx_row, sy_row, sz_ref, sx_col, sy_col,
    load_sem, v_sem, row_send, row_recv, first_recv, col_send, col_recv, last_recv, raw_send, raw_recv, raw_near,
):
    rows, cols, chunks, per, lag, lanes = dims
    part_y, part_z = v.shape[1], v.shape[2]
    grid_x, grid_y = v.shape[0], rbuf.shape[1]
    share_y, grid_z = zbuf.shape[1], zbuf.shape[2]
    tiles, tile = t.shape[1], t.shape[3]
    r, c = lax.axis_index("row"), lax.axis_index("col")
    spans = [pl.ds(p * lanes, lanes) for p in range(part_z // lanes)]

    load_w = pltpu.make_async_copy(w_hbm.at[0], w.at[0], load_sem.at[1])
    load_rest = pltpu.make_async_copy(w_hbm.at[pl.ds(1, chunks - 1)], w.at[pl.ds(1, chunks - 1)], load_sem.at[2])
    load_t = pltpu.make_async_copy(t_hbm, t, load_sem.at[0])
    load_v = [
        pltpu.make_async_copy(v_hbm.at[:, :, span], v.at[:, :, span], v_sem.at[p])
        for p, span in enumerate(spans)
    ]
    load_symbols = [
        pltpu.make_async_copy(source, target, load_sem.at[3 + n])
        for n, (source, target) in enumerate(((sx_hbm, sx_row), (sy_hbm, sy_row), (sz_hbm, sz_ref)))
    ]
    half = cols // 2
    side = c // half
    row_masks = sorted(range(1, rows), key=lambda m: (-bin(m // 2).count("1"), m))
    row_peers = [flipped(r, m) for m in row_masks]
    near = [flipped(c, m) for m in range(1, half)]
    across = [(half + j) * (1 - side) + (half - 1 - j) * side for j in reversed(range(half))]
    col_peers = near + across
    mirror = cols - 1 - c
    depth = (half - 1 - c) * (1 - side) + (c - half) * side
    marks = list(range(half - 1)) + [2 * half - 2 - depth] * half
    col_targets = list(zip(col_peers, marks))

    barrier = pltpu.get_barrier_semaphore()
    for s in row_peers:
        pl.semaphore_signal(barrier, inc=1, device_id=(s, c), device_id_type=MESH)
    for s in col_peers:
        pl.semaphore_signal(barrier, inc=1, device_id=(r, s), device_id_type=MESH)
    load_w.start()
    for load in load_v + load_symbols:
        load.start()

    step = SUB * SUB
    whole = pl.ds(0, part_z)
    ends, done = [], 0
    while done < part_z:
        left = part_z - done
        ends.append(pl.ds(done, left // 2 if left % 256 == 0 and len(ends) < 2 else left))
        done += ends[-1].size

    def split_parts(span):
        def part_loop(i, carry):
            for g in range(part_y // SUB):
                block = v[pl.ds(i * SUB, SUB), g * SUB:(g + 1) * SUB, span].reshape(step, lanes)
                high, low = split(block)
                v_parts[g, 0, pl.ds(pl.multiple_of(i * step, step), step), span] = high
                v_parts[g, 1, pl.ds(pl.multiple_of(i * step, step), step), span] = low
            return carry

        lax.fori_loop(0, grid_x // SUB, part_loop, 0)

    def x_stage(k, span):
        m, depth = rows * per * SUB, grid_x * SUB
        for g in range(part_y // SUB):
            both = product(w[k, :2 * m, :depth], v_parts[g, 0, :, span])
            sums = both[:m] + both[m:] + product(w[k, :m, :depth], v_parts[g, 1, :, span])
            xs[k, :, g * SUB:(g + 1) * SUB, span] = sums.reshape(rows * per, SUB, span.size)

    def own_rows():
        return pl.ds(pl.multiple_of(r * part_y, SUB), part_y)

    def row_stage(k, span, recv):
        for i in range(per):
            for s in row_peers:
                pltpu.make_async_remote_copy(
                    src_ref=xs.at[k, s * per + i, :, span],
                    dst_ref=rbuf.at[k * per + i, own_rows(), span],
                    send_sem=row_send, recv_sem=recv.at[i],
                    device_id=(s, c), device_id_type=MESH,
                ).start()
        rbuf[pl.ds(k * per, per), own_rows(), span] = xs[k, pl.ds(r * per, per), :, span]

    def y_plane(k, i, span, recv):
        came = rbuf.at[k * per + i, pl.ds(0, grid_y - part_y), span]
        pltpu.make_async_copy(came, came, recv.at[i]).wait()
        high, low = split(rbuf[k * per + i, :, span])
        both = product(w[0, :2 * grid_y, grid_x * SUB:], high)
        ybuf[k, i, :, span] = both[:grid_y] + both[grid_y:] + product(w[0, :grid_y, grid_x * SUB:], low)

    def col_stage(k, i, span, recv, targets):
        at = pl.ds(pl.multiple_of(c * part_z + span.start, 128), span.size)
        for s, mark in targets:
            pltpu.make_async_remote_copy(
                src_ref=ybuf.at[k, i, pl.ds(pl.multiple_of(s * share_y, SUB), share_y), span],
                dst_ref=zbuf.at[k * per + i, :, at],
                send_sem=col_send, recv_sem=recv.at[mark],
                device_id=(r, s), device_id_type=MESH,
            ).start()

    def y_stage(k, span, recv, raw=False):
        for i in range(per):
            y_plane(k, i, span, recv)
            near_only = raw and i == per - 1
            col_stage(k, i, span, col_recv.at[k], col_targets[:len(near)] if near_only else col_targets)

    def raw_stage():
        for s in range(rows):
            pltpu.make_async_remote_copy(
                src_ref=xs.at[0, s * per + per - 1, :, spans[0]], dst_ref=raw_in.at[s],
                send_sem=raw_send.at[0], recv_sem=raw_recv.at[0],
                device_id=(r, mirror), device_id_type=MESH,
            ).start()

    def raw_row_stage():
        pltpu.make_async_copy(raw_in, raw_in, raw_recv.at[0]).wait()
        for s in row_peers:
            pltpu.make_async_remote_copy(
                src_ref=raw_in.at[s], dst_ref=raw_all.at[own_rows(), :],
                send_sem=raw_send.at[1], recv_sem=raw_recv.at[1],
                device_id=(s, c), device_id_type=MESH,
            ).start()
        raw_all[own_rows(), :] = raw_in[r]

    def raw_y_stage():
        came = raw_all.at[pl.ds(0, grid_y - part_y), :]
        pltpu.make_async_copy(came, came, raw_recv.at[1]).wait()
        high, low = split(raw_all[...])
        both = product(w[0, :2 * grid_y, grid_x * SUB:], high)
        raw_y[...] = both[:grid_y] + both[grid_y:] + product(w[0, :grid_y, grid_x * SUB:], low)
        at = pl.ds(pl.multiple_of(mirror * part_z, 128), lanes)
        for m, s in enumerate(near):
            pltpu.make_async_remote_copy(
                src_ref=raw_y.at[pl.ds(pl.multiple_of(s * share_y, SUB), share_y), :],
                dst_ref=zbuf.at[per - 1, :, at],
                send_sem=raw_send.at[2], recv_sem=raw_near.at[m],
                device_id=(r, s), device_id_type=MESH,
            ).start()
        zbuf[per - 1, :, at] = raw_y[pl.ds(pl.multiple_of(c * share_y, SUB), share_y), :]

    def last_y_stage(k, recv):
        for i in range(per):
            y_plane(k, i, whole, recv)
        for target in col_targets:
            for q, span in enumerate(ends):
                for i in range(per):
                    col_stage(k, i, span, last_recv.at[q], [target])

    def own_z(k):
        zbuf[pl.ds(k * per, per), :, pl.ds(pl.multiple_of(c * part_z, 128), part_z)] = (
            ybuf[k, :, pl.ds(pl.multiple_of(c * share_y, SUB), share_y), :]
        )

    def col_wait(k, m):
        came = zbuf.at[pl.ds(k * per, per), :, pl.ds(0, part_z)]
        pltpu.make_async_copy(came, came, col_recv.at[k, m]).wait()

    def factor_parts(k, n):
        y_part = sy_col[pl.ds(pl.multiple_of(c * share_y, SUB), share_y), :]
        z_part = sz_ref[:, pl.ds(pl.multiple_of(n * tile, tile), tile)]
        plane = jnp.concatenate([y_part] * (tile // 128), axis=1) + z_part
        for i in range(per):
            x_part = sx_col[pl.ds(r * chunks * per + k * per + i, 1), :]
            symbol = jnp.concatenate([x_part] * (tile // 128), axis=1) + plane
            yield i, (1.0 - 0.2 * symbol) / (1.0 + 0.2 * symbol)

    size = per * share_y

    def scaled(k, n, sums):
        for i, factor in factor_parts(k, n):
            out_ref[k * per + i, :, pl.ds(pl.multiple_of(n * tile, tile), tile)] = (
                sums[i * share_y:(i + 1) * share_y] * factor
            )

    def z_part(k, start, count, finish=None, first=False):
        span = pl.ds(pl.multiple_of(start, 128), count)
        high, low = split(zbuf[pl.ds(k * per, per), :, span].reshape(size, count))
        lhs[:size, :count] = high
        lhs[size:, :count] = low

        def tile_loop(n, carry):
            both = product(lhs[:, :count], t[0, n, span, :])
            sums = both[:size] + both[size:] + product(lhs[:size, :count], t[1, n, span, :])
            at = pl.ds(pl.multiple_of(n * tile, tile), tile)
            if not first:
                sums = sums + out_ref[pl.ds(k * per, per), :, at].reshape(size, tile)
            if finish is None:
                out_ref[pl.ds(k * per, per), :, at] = sums.reshape(per, share_y, tile)
            else:
                finish(k, n, sums)
            return carry

        lax.fori_loop(0, tiles, tile_loop, 0, unroll=8 if count <= 256 else 4)

    def prepare(k):
        def tile_loop(n, carry):
            for i, factor in factor_parts(k, n):
                factors[i, :, pl.ds(pl.multiple_of(n * tile, tile), tile)] = factor
            return carry

        lax.fori_loop(0, tiles, tile_loop, 0)

    def multiplied(k, n, sums):
        at = pl.ds(pl.multiple_of(n * tile, tile), tile)
        out_ref[pl.ds(k * per, per), :, at] = sums.reshape(per, share_y, tile) * factors[:, :, at]

    def last_wait(q, m):
        came = zbuf.at[pl.ds((chunks - 1) * per, per), :, pl.ds(0, ends[q].size)]
        pltpu.make_async_copy(came, came, last_recv.at[q, m]).wait()

    def own_stage(k):
        for m in range(len(near)):
            col_wait(k, m)
        z_part(k, side * half * part_z, half * part_z, first=True)

    def across_stage(k):
        @pl.when(k == 0)
        def _():
            for m in range(len(near), len(col_peers)):
                came = zbuf.at[0, :, pl.ds(0, per * part_z - lanes)]
                pltpu.make_async_copy(came, came, col_recv.at[0, m]).wait()
            for m in range(len(near)):
                came = zbuf.at[0, :, pl.ds(0, lanes)]
                pltpu.make_async_copy(came, came, raw_near.at[m]).wait()

        @pl.when(k > 0)
        def _():
            for m in range(len(near), len(col_peers)):
                col_wait(k, m)

        z_part(k, (1 - side) * half * part_z, half * part_z, scaled)

    def last_stages():
        before, last = chunks - 2, chunks - 1
        for m in range(len(near)):
            for q in range(len(ends)):
                last_wait(q, m)
        z_part(last, side * half * part_z, half * part_z, first=True)
        prepare(last)
        for j in range(half - 1):
            col_wait(before, len(near) + j)
            z_part(before, across[j] * part_z, part_z)
        for j in range(half - 1):
            for q in range(len(ends)):
                last_wait(q, len(near) + j)
            z_part(last, across[j] * part_z, part_z)
        col_wait(before, len(col_peers) - 1)
        z_part(before, across[-1] * part_z, part_z, scaled)
        for q, span in enumerate(ends):
            last_wait(q, len(col_peers) - 1)
            z_part(last, across[-1] * part_z + span.start, span.size, multiplied if q == len(ends) - 1 else None)

    for p, span in enumerate(spans):
        load_v[p].wait()
        split_parts(span)
        if p == 0:
            load_w.wait()
        x_stage(0, span)
        if p == 0:
            pl.semaphore_wait(barrier, len(row_peers) + len(col_peers))
        row_stage(0, span, first_recv.at[p])
        if p == 0:
            raw_stage()
    load_rest.start()
    load_t.start()
    y_stage(0, spans[0], first_recv.at[0], raw=True)
    load_rest.wait()
    x_stage(1, whole)
    row_stage(1, whole, row_recv.at[1])
    for p, span in enumerate(spans[1:]):
        y_stage(0, span, first_recv.at[p + 1])
    own_z(0)
    raw_row_stage()
    for load in load_symbols:
        load.wait()
    for ref, column in ((sx_row, sx_col), (sy_row, sy_col)):
        column[...] = jnp.broadcast_to(ref[...], (128, ref.shape[1])).T

    def loop(k, carry):
        @pl.when(k < chunks)
        def _():
            x_stage(k, whole)
            row_stage(k, whole, row_recv.at[k])

        @pl.when(k < chunks)
        def _():
            y_stage(k - 1, whole, row_recv.at[k - 1])
            own_z(k - 1)

        @pl.when(k == chunks)
        def _():
            last_y_stage(chunks - 1, row_recv.at[chunks - 1])
            own_z(chunks - 1)

        @pl.when(k == 2)
        def _():
            raw_y_stage()
            load_t.wait()

        own_stage(k - lag)

        @pl.when(k >= lag + 1)
        def _():
            across_stage(k - 1 - lag)

        return carry

    lax.fori_loop(2, chunks + lag - 1, loop, 0)
    last_stages()

    sent = rbuf.at[:, pl.ds(0, grid_y - part_y), :]
    pltpu.make_async_copy(sent, sent, row_send).wait()
    pltpu.make_async_copy(raw_in, raw_in, raw_send.at[0]).wait()
    sent = raw_all.at[pl.ds(0, grid_y - part_y), :]
    pltpu.make_async_copy(sent, sent, raw_send.at[1]).wait()
    if near:
        sent = raw_y.at[pl.ds(0, len(near) * share_y), :]
        pltpu.make_async_copy(sent, sent, raw_send.at[2]).wait()
    for sent in (
        zbuf.at[pl.ds(1, grid_x // rows - 1), :, pl.ds(0, grid_z - part_z)],
        zbuf.at[0, :, pl.ds(0, grid_z - part_z - half * lanes)],
    ):
        pltpu.make_async_copy(sent, sent, col_send).wait()


def transformed(rows, cols, velocity, symbol_x, symbol_y, symbol_z):
    grid_x, part_y, part_z = velocity.shape
    grid_y, grid_z = part_y * rows, part_z * cols
    share_x, share_y = grid_x // rows, grid_y // cols
    chunks = min(8, share_x)
    per = share_x // chunks
    tile = 256
    hx, hy, hz = fixed_table(grid_x), fixed_table(grid_y), fixed_table(grid_z)
    order = np.arange(grid_x).reshape(rows, chunks, per).transpose(1, 0, 2).reshape(chunks, rows * per)
    w = np.stack([np.kron(hx[o], np.eye(SUB, dtype=np.float32)) for o in order])
    w = np.concatenate(halves(w), axis=1)
    h = np.concatenate(halves(hy), axis=0)
    t = np.stack(halves(hz)).reshape(2, grid_z, grid_z // tile, tile).transpose(0, 2, 1, 3)
    held = np.zeros((chunks, max(w.shape[1], h.shape[0]), w.shape[2] + h.shape[1]), w.dtype)
    held[:, :w.shape[1], :w.shape[2]] = w
    held[0, :h.shape[0], w.shape[2]:] = h
    f32, bf16 = jnp.float32, jnp.bfloat16
    hbm = pl.BlockSpec(memory_space=pltpu.HBM)
    vmem = pl.BlockSpec(memory_space=pltpu.VMEM)
    return pl.pallas_call(
        functools.partial(kernel, (rows, cols, chunks, per, 2, 128)),
        out_shape=jax.ShapeDtypeStruct((share_x, share_y, grid_z), f32),
        in_specs=[hbm] * 6,
        out_specs=vmem,
        scratch_shapes=[
            pltpu.VMEM(velocity.shape, f32),
            pltpu.VMEM(held.shape, bf16),
            pltpu.VMEM(t.shape, bf16),
            pltpu.VMEM((part_y // SUB, 2, grid_x * SUB, part_z), bf16),
            pltpu.VMEM((chunks, rows * per, part_y, part_z), f32),
            pltpu.VMEM((share_x, grid_y, part_z), f32),
            pltpu.VMEM((chunks, per, grid_y, part_z), f32),
            pltpu.VMEM((share_x, share_y, grid_z), f32),
            pltpu.VMEM((2 * per * share_y, grid_z), bf16),
            pltpu.VMEM((per, share_y, grid_z), f32),
            pltpu.VMEM((rows, part_y, 128), f32),
            pltpu.VMEM((grid_y, 128), f32),
            pltpu.VMEM((grid_y, 128), f32),
            pltpu.VMEM((1, grid_x), f32),
            pltpu.VMEM((1, grid_y), f32),
            pltpu.VMEM((1, grid_z), f32),
            pltpu.VMEM((grid_x, 128), f32),
            pltpu.VMEM((grid_y, 128), f32),
            pltpu.SemaphoreType.DMA((6,)),
            pltpu.SemaphoreType.DMA((part_z // 128,)),
            pltpu.SemaphoreType.DMA,
            pltpu.SemaphoreType.DMA((chunks, per)),
            pltpu.SemaphoreType.DMA((part_z // 128, per)),
            pltpu.SemaphoreType.DMA,
            pltpu.SemaphoreType.DMA((chunks, cols - 1)),
            pltpu.SemaphoreType.DMA((3, cols - 1)),
            pltpu.SemaphoreType.DMA((3,)),
            pltpu.SemaphoreType.DMA((2,)),
            pltpu.SemaphoreType.DMA((max(1, cols // 2 - 1),)),
        ],
        compiler_params=pltpu.CompilerParams(
            collective_id=0, has_side_effects=True, vmem_limit_bytes=47 * 2**20
        ),
    )(velocity, jnp.asarray(held), jnp.asarray(np.ascontiguousarray(t)),
      *(pltpu.with_memory_space_constraint(symbol[None, :], pltpu.HBM) for symbol in (symbol_x, symbol_y, symbol_z)))


def fits(rows, cols, shape):
    grid_x, part_y, part_z = shape
    grid_z = part_z * cols
    held = 7 * grid_x * part_y * part_z * 4 + 4 * grid_z * grid_z + 4 * (grid_x * SUB) ** 2
    even = rows & (rows - 1) == 0 and cols & (cols - 1) == 0 and cols > 1 and grid_x % (16 * rows) == 0
    even = even and grid_x * part_z <= 8 * rows * grid_z
    return even and part_y % SUB == 0 and part_z % 128 == 0 and (part_y * rows) % (SUB * cols) == 0 and held < 54 * 2**20


def local(rows, cols, velocity, symbol_x, symbol_y, symbol_z):
    if fits(rows, cols, velocity.shape):
        return transformed(rows, cols, velocity, symbol_x, symbol_y, symbol_z)
    part_values = along_dim(velocity, 0)
    part_values = lax.all_to_all(part_values, "row", split_axis=0, concat_axis=1, tiled=True)
    pencil_values = along_dim(part_values, 1)
    pencil_values = lax.all_to_all(pencil_values, "col", split_axis=1, concat_axis=2, tiled=True)
    pencil_values = along_dim(pencil_values, 2)
    share_x = pencil_values.shape[0]
    part_x = lax.dynamic_slice_in_dim(symbol_x, lax.axis_index("row") * share_x, share_x)
    share_y = pencil_values.shape[1]
    part_y = lax.dynamic_slice_in_dim(symbol_y, lax.axis_index("col") * share_y, share_y)
    symbol = part_x[:, None, None] + part_y[None, :, None] + symbol_z[None, None, :]
    return pencil_values * ((1.0 - 0.2 * symbol) / (1.0 + 0.2 * symbol))


def solution(mesh):
    placed = (P(None, "row", "col"), P(), P(), P())
    return jax.shard_map(
        functools.partial(local, mesh.shape["row"], mesh.shape["col"]),
        mesh=mesh, in_specs=placed, out_specs=P("row", "col", None), check_vma=False,
    )
```

```python
import functools

import jax
import jax.numpy as jnp
import numpy as np
from jax import lax
from jax.experimental import pallas as pl
from jax.experimental.pallas import tpu as pltpu
from jax.sharding import PartitionSpec as P

SUB = 8
MESH = pl.DeviceIdType.MESH


def mode_table(count):
    rank = jnp.arange(count)
    angle = 2.0 * jnp.pi / count * (rank[:, None] * rank[None, :] % count).astype(jnp.float32)
    return (jnp.cos(angle) + jnp.sin(angle)) * count ** (-0.5)


def along_dim(values, dim):
    moved = jnp.tensordot(
        values, mode_table(values.shape[dim]), axes=([dim], [0]), precision=lax.Precision.HIGHEST
    )
    return jnp.moveaxis(moved, -1, dim)


def fixed_table(count):
    rank = np.arange(count)
    angle = 2.0 * np.pi / count * (rank[:, None] * rank[None, :] % count)
    return ((np.cos(angle) + np.sin(angle)) * count ** (-0.5)).astype(np.float32)


def halves(table):
    high = table.astype(jnp.bfloat16)
    low = (table - high.astype(np.float32)).astype(jnp.bfloat16)
    return high, low


def split(values):
    high = values.astype(jnp.bfloat16)
    low = (values - high.astype(jnp.float32)).astype(jnp.bfloat16)
    return high, low


def product(a, b):
    return jnp.dot(a, b, preferred_element_type=jnp.float32)


def flipped(index, mask):
    out = index
    bit = 1
    while bit <= mask:
        if mask & bit:
            out = out + bit * (1 - 2 * ((index // bit) % 2))
        bit *= 2
    return out


def kernel(
    dims, v_hbm, w_hbm, t_hbm, sx_hbm, sy_hbm, sz_hbm, out_ref,
    v, w, t, v_parts, xs, rbuf, ybuf, zbuf, lhs, factors, raw_in, raw_all, raw_y, sx_row, sy_row, sz_ref, sx_col, sy_col,
    load_sem, v_sem, sent_sem, row_recv, first_recv, col_recv, last_recv, raw_recv, raw_near,
):
    rows, cols, chunks, per, lag, lanes, raws = dims
    raw = raws * lanes
    part_y, part_z = v.shape[1], v.shape[2]
    grid_x, grid_y = v.shape[0], rbuf.shape[1]
    share_y, grid_z = zbuf.shape[1], zbuf.shape[2]
    tiles, tile = t.shape[1], t.shape[3]
    r, c = lax.axis_index("row"), lax.axis_index("col")
    spans = [pl.ds(p * lanes, lanes) for p in range(part_z // lanes)]

    load_w = pltpu.make_async_copy(w_hbm.at[0], w.at[0], load_sem.at[1])
    load_rest = pltpu.make_async_copy(w_hbm.at[pl.ds(1, chunks - 1)], w.at[pl.ds(1, chunks - 1)], load_sem.at[2])
    load_t = pltpu.make_async_copy(t_hbm, t, load_sem.at[0])
    groups = [pl.ds(g * SUB, SUB) for g in range(part_y // SUB)]
    parts = [(group, spans[0]) for group in groups] + [(pl.ds(0, part_y), span) for span in spans[1:]]
    load_v = [
        pltpu.make_async_copy(v_hbm.at[:, y, z], v.at[:, y, z], v_sem.at[p]) for p, (y, z) in enumerate(parts)
    ]
    load_symbols = [
        pltpu.make_async_copy(source, target, load_sem.at[3 + n])
        for n, (source, target) in enumerate(((sx_hbm, sx_row), (sy_hbm, sy_row), (sz_hbm, sz_ref)))
    ]
    half = cols // 2
    side = c // half
    row_masks = sorted(range(1, rows), key=lambda m: (-bin(m // 2).count("1"), m))
    row_peers = [flipped(r, m) for m in row_masks]
    near = [flipped(c, m) for m in range(1, half)]
    across = [(half + j) * (1 - side) + (half - 1 - j) * side for j in reversed(range(half))]
    col_peers = near + across
    mirror = cols - 1 - c
    depth = (half - 1 - c) * (1 - side) + (c - half) * side
    marks = list(range(half - 1)) + [2 * half - 2 - depth] * half
    col_targets = list(zip(col_peers, marks))

    barrier = pltpu.get_barrier_semaphore()
    for s in row_peers:
        pl.semaphore_signal(barrier, inc=1, device_id=(s, c), device_id_type=MESH)
    for s in col_peers:
        pl.semaphore_signal(barrier, inc=1, device_id=(r, s), device_id_type=MESH)
    load_w.start()
    for load in load_v + load_symbols:
        load.start()

    step = SUB * SUB
    whole = pl.ds(0, part_z)
    ends, done = [], 0
    while done < part_z:
        left = part_z - done
        ends.append(pl.ds(done, left // 2 if left % 256 == 0 and len(ends) < 2 else left))
        done += ends[-1].size

    def split_parts(span, picked):
        def part_loop(i, carry):
            for g in picked:
                block = v[pl.ds(i * SUB, SUB), g * SUB:(g + 1) * SUB, span].reshape(step, lanes)
                high, low = split(block)
                v_parts[g, 0, pl.ds(pl.multiple_of(i * step, step), step), span] = high
                v_parts[g, 1, pl.ds(pl.multiple_of(i * step, step), step), span] = low
            return carry

        lax.fori_loop(0, grid_x // SUB, part_loop, 0)

    def x_stage(k, span, picked):
        m, depth = rows * per * SUB, grid_x * SUB
        for g in picked:
            both = product(w[k, :2 * m, :depth], v_parts[g, 0, :, span])
            sums = both[:m] + both[m:] + product(w[k, :m, :depth], v_parts[g, 1, :, span])
            xs[k, :, g * SUB:(g + 1) * SUB, span] = sums.reshape(rows * per, SUB, span.size)

    def own_rows():
        return pl.ds(pl.multiple_of(r * part_y, SUB), part_y)

    def row_stage(k, span, recv):
        for i in range(per):
            for s in row_peers:
                pltpu.make_async_remote_copy(
                    src_ref=xs.at[k, s * per + i, :, span],
                    dst_ref=rbuf.at[k * per + i, own_rows(), span],
                    send_sem=sent_sem, recv_sem=recv.at[i],
                    device_id=(s, c), device_id_type=MESH,
                ).start()
        rbuf[pl.ds(k * per, per), own_rows(), span] = xs[k, pl.ds(r * per, per), :, span]

    def y_plane(k, i, span, recv):
        came = rbuf.at[k * per + i, pl.ds(0, grid_y - part_y), span]
        pltpu.make_async_copy(came, came, recv.at[i]).wait()
        high, low = split(rbuf[k * per + i, :, span])
        both = product(w[0, :2 * grid_y, grid_x * SUB:], high)
        ybuf[k, i, :, span] = both[:grid_y] + both[grid_y:] + product(w[0, :grid_y, grid_x * SUB:], low)

    def col_stage(k, i, span, recv, targets):
        at = pl.ds(pl.multiple_of(c * part_z + span.start, 128), span.size)
        for s, mark in targets:
            pltpu.make_async_remote_copy(
                src_ref=ybuf.at[k, i, pl.ds(pl.multiple_of(s * share_y, SUB), share_y), span],
                dst_ref=zbuf.at[k * per + i, :, at],
                send_sem=sent_sem, recv_sem=recv.at[mark],
                device_id=(r, s), device_id_type=MESH,
            ).start()

    def y_stage(k, span, recv, crossed=False):
        for i in range(per):
            y_plane(k, i, span, recv)
            near_only = crossed and i == per - 1
            col_stage(k, i, span, col_recv.at[k], col_targets[:len(near)] if near_only else col_targets)

    def raw_stage(span):
        for s in range(rows):
            pltpu.make_async_remote_copy(
                src_ref=xs.at[0, s * per + per - 1, :, span], dst_ref=raw_in.at[s, :, span],
                send_sem=sent_sem, recv_sem=raw_recv.at[0],
                device_id=(r, mirror), device_id_type=MESH,
            ).start()

    def raw_row_stage():
        pltpu.make_async_copy(raw_in, raw_in, raw_recv.at[0]).wait()
        for s in row_peers:
            pltpu.make_async_remote_copy(
                src_ref=raw_in.at[s], dst_ref=raw_all.at[own_rows(), :],
                send_sem=sent_sem, recv_sem=raw_recv.at[1],
                device_id=(s, c), device_id_type=MESH,
            ).start()
        raw_all[own_rows(), :] = raw_in[r]

    def raw_y_stage():
        came = raw_all.at[pl.ds(0, grid_y - part_y), :]
        pltpu.make_async_copy(came, came, raw_recv.at[1]).wait()
        high, low = split(raw_all[...])
        both = product(w[0, :2 * grid_y, grid_x * SUB:], high)
        raw_y[...] = both[:grid_y] + both[grid_y:] + product(w[0, :grid_y, grid_x * SUB:], low)
        at = pl.ds(pl.multiple_of(mirror * part_z, 128), raw)
        for m, s in enumerate(near):
            pltpu.make_async_remote_copy(
                src_ref=raw_y.at[pl.ds(pl.multiple_of(s * share_y, SUB), share_y), :],
                dst_ref=zbuf.at[per - 1, :, at],
                send_sem=sent_sem, recv_sem=raw_near.at[m],
                device_id=(r, s), device_id_type=MESH,
            ).start()
        zbuf[per - 1, :, at] = raw_y[pl.ds(pl.multiple_of(c * share_y, SUB), share_y), :]

    def last_y_stage(k, recv):
        for i in range(per):
            y_plane(k, i, whole, recv)
        for target in col_targets:
            for q, span in enumerate(ends):
                for i in range(per):
                    col_stage(k, i, span, last_recv.at[q], [target])

    def own_z(k):
        zbuf[pl.ds(k * per, per), :, pl.ds(pl.multiple_of(c * part_z, 128), part_z)] = (
            ybuf[k, :, pl.ds(pl.multiple_of(c * share_y, SUB), share_y), :]
        )

    def col_wait(k, m):
        came = zbuf.at[pl.ds(k * per, per), :, pl.ds(0, part_z)]
        pltpu.make_async_copy(came, came, col_recv.at[k, m]).wait()

    def factor_parts(k, n):
        y_part = sy_col[pl.ds(pl.multiple_of(c * share_y, SUB), share_y), :]
        z_part = sz_ref[:, pl.ds(pl.multiple_of(n * tile, tile), tile)]
        plane = jnp.concatenate([y_part] * (tile // 128), axis=1) + z_part
        for i in range(per):
            x_part = sx_col[pl.ds(r * chunks * per + k * per + i, 1), :]
            symbol = jnp.concatenate([x_part] * (tile // 128), axis=1) + plane
            yield i, (1.0 - 0.2 * symbol) / (1.0 + 0.2 * symbol)

    size = per * share_y

    def scaled(k, n, sums):
        for i, factor in factor_parts(k, n):
            out_ref[k * per + i, :, pl.ds(pl.multiple_of(n * tile, tile), tile)] = (
                sums[i * share_y:(i + 1) * share_y] * factor
            )

    def z_part(k, start, count, finish=None, first=False):
        span = pl.ds(pl.multiple_of(start, 128), count)
        high, low = split(zbuf[pl.ds(k * per, per), :, span].reshape(size, count))
        lhs[:size, :count] = high
        lhs[size:, :count] = low

        def tile_loop(n, carry):
            both = product(lhs[:, :count], t[0, n, span, :])
            sums = both[:size] + both[size:] + product(lhs[:size, :count], t[1, n, span, :])
            at = pl.ds(pl.multiple_of(n * tile, tile), tile)
            if not first:
                sums = sums + out_ref[pl.ds(k * per, per), :, at].reshape(size, tile)
            if finish is None:
                out_ref[pl.ds(k * per, per), :, at] = sums.reshape(per, share_y, tile)
            else:
                finish(k, n, sums)
            return carry

        lax.fori_loop(0, tiles, tile_loop, 0, unroll=8 if count <= 256 else 4)

    def prepare(k):
        def tile_loop(n, carry):
            for i, factor in factor_parts(k, n):
                factors[i, :, pl.ds(pl.multiple_of(n * tile, tile), tile)] = factor
            return carry

        lax.fori_loop(0, tiles, tile_loop, 0)

    def multiplied(k, n, sums):
        at = pl.ds(pl.multiple_of(n * tile, tile), tile)
        out_ref[pl.ds(k * per, per), :, at] = sums.reshape(per, share_y, tile) * factors[:, :, at]

    def last_wait(q, m):
        came = zbuf.at[pl.ds((chunks - 1) * per, per), :, pl.ds(0, ends[q].size)]
        pltpu.make_async_copy(came, came, last_recv.at[q, m]).wait()

    def own_stage(k):
        for m in range(len(near)):
            col_wait(k, m)
        z_part(k, side * half * part_z, half * part_z, first=True)

    def across_stage(k):
        @pl.when(k == 0)
        def _():
            for m in range(len(near), len(col_peers)):
                came = zbuf.at[0, :, pl.ds(0, per * part_z - raw)]
                pltpu.make_async_copy(came, came, col_recv.at[0, m]).wait()
            for m in range(len(near)):
                came = zbuf.at[0, :, pl.ds(0, raw)]
                pltpu.make_async_copy(came, came, raw_near.at[m]).wait()

        @pl.when(k > 0)
        def _():
            for m in range(len(near), len(col_peers)):
                col_wait(k, m)

        z_part(k, (1 - side) * half * part_z, half * part_z, scaled)

    def last_stages():
        before, last = chunks - 2, chunks - 1
        for m in range(len(near)):
            for q in range(len(ends)):
                last_wait(q, m)
        z_part(last, side * half * part_z, half * part_z, first=True)
        prepare(last)
        for j in range(half - 1):
            col_wait(before, len(near) + j)
            z_part(before, across[j] * part_z, part_z)
        for j in range(half - 1):
            for q in range(len(ends)):
                last_wait(q, len(near) + j)
            z_part(last, across[j] * part_z, part_z)
        col_wait(before, len(col_peers) - 1)
        z_part(before, across[-1] * part_z, part_z, scaled)
        for q, span in enumerate(ends):
            last_wait(q, len(col_peers) - 1)
            z_part(last, across[-1] * part_z + span.start, span.size, multiplied if q == len(ends) - 1 else None)

    every = range(len(groups))
    for p, load in enumerate(load_v):
        load.wait()
        n = max(0, p + 1 - len(groups))
        picked = [p] if p < len(groups) else every
        split_parts(spans[n], picked)
        if p == 0:
            load_w.wait()
        x_stage(0, spans[n], picked)
        if p + 1 < len(groups):
            continue
        if n == 0:
            pl.semaphore_wait(barrier, len(row_peers) + len(col_peers))
        row_stage(0, spans[n], first_recv.at[n])
        if n < raws:
            raw_stage(spans[n])
    load_rest.start()
    load_t.start()
    for p, span in enumerate(spans):
        if p == min(2, len(spans) - 1):
            load_rest.wait()
            x_stage(1, whole, every)
            row_stage(1, whole, row_recv.at[0])
        y_stage(0, span, first_recv.at[p], crossed=p < raws)
    own_z(0)
    raw_row_stage()
    for load in load_symbols:
        load.wait()
    for ref, column in ((sx_row, sx_col), (sy_row, sy_col)):
        column[...] = jnp.broadcast_to(ref[...], (128, ref.shape[1])).T

    def loop(k, carry):
        @pl.when(k < chunks)
        def _():
            x_stage(k, whole, every)
            row_stage(k, whole, row_recv.at[k - 1])

        @pl.when(k < chunks)
        def _():
            y_stage(k - 1, whole, row_recv.at[k - 2])
            own_z(k - 1)

        @pl.when(k == chunks)
        def _():
            last_y_stage(chunks - 1, row_recv.at[chunks - 2])
            own_z(chunks - 1)

        @pl.when(k == 2)
        def _():
            raw_y_stage()
            load_t.wait()

        own_stage(k - lag)

        @pl.when(k >= lag + 1)
        def _():
            across_stage(k - 1 - lag)

        return carry

    lax.fori_loop(2, chunks + lag - 1, loop, 0)
    last_stages()

    sent = [
        rbuf.at[:, pl.ds(0, grid_y - part_y), :],
        raw_in,
        raw_all.at[pl.ds(0, grid_y - part_y), :],
        zbuf.at[pl.ds(1, grid_x // rows - 1), :, pl.ds(0, grid_z - part_z)],
        zbuf.at[0, :, pl.ds(0, grid_z - part_z - half * raw)],
    ]
    if near:
        sent.append(raw_y.at[pl.ds(0, len(near) * share_y), :])
    for ref in sent:
        pltpu.make_async_copy(ref, ref, sent_sem).wait()


def transformed(rows, cols, velocity, symbol_x, symbol_y, symbol_z):
    grid_x, part_y, part_z = velocity.shape
    grid_y, grid_z = part_y * rows, part_z * cols
    share_x, share_y = grid_x // rows, grid_y // cols
    chunks, raws = min(8, share_x), 1
    per = share_x // chunks
    tile = 256
    hx, hy, hz = fixed_table(grid_x), fixed_table(grid_y), fixed_table(grid_z)
    order = np.arange(grid_x).reshape(rows, chunks, per).transpose(1, 0, 2).reshape(chunks, rows * per)
    w = np.stack([np.kron(hx[o], np.eye(SUB, dtype=np.float32)) for o in order])
    w = np.concatenate(halves(w), axis=1)
    h = np.concatenate(halves(hy), axis=0)
    t = np.stack(halves(hz)).reshape(2, grid_z, grid_z // tile, tile).transpose(0, 2, 1, 3)
    held = np.zeros((chunks, max(w.shape[1], h.shape[0]), w.shape[2] + h.shape[1]), w.dtype)
    held[:, :w.shape[1], :w.shape[2]] = w
    held[0, :h.shape[0], w.shape[2]:] = h
    f32, bf16 = jnp.float32, jnp.bfloat16
    hbm = pl.BlockSpec(memory_space=pltpu.HBM)
    vmem = pl.BlockSpec(memory_space=pltpu.VMEM)
    return pl.pallas_call(
        functools.partial(kernel, (rows, cols, chunks, per, 2, 128, raws)),
        out_shape=jax.ShapeDtypeStruct((share_x, share_y, grid_z), f32),
        in_specs=[hbm] * 6,
        out_specs=vmem,
        scratch_shapes=[
            pltpu.VMEM(velocity.shape, f32),
            pltpu.VMEM(held.shape, bf16),
            pltpu.VMEM(t.shape, bf16),
            pltpu.VMEM((part_y // SUB, 2, grid_x * SUB, part_z), bf16),
            pltpu.VMEM((chunks, rows * per, part_y, part_z), f32),
            pltpu.VMEM((share_x, grid_y, part_z), f32),
            pltpu.VMEM((chunks, per, grid_y, part_z), f32),
            pltpu.VMEM((share_x, share_y, grid_z), f32),
            pltpu.VMEM((2 * per * share_y, grid_z), bf16),
            pltpu.VMEM((per, share_y, grid_z), f32),
            pltpu.VMEM((rows, part_y, raws * 128), f32),
            pltpu.VMEM((grid_y, raws * 128), f32),
            pltpu.VMEM((grid_y, raws * 128), f32),
            pltpu.VMEM((1, grid_x), f32),
            pltpu.VMEM((1, grid_y), f32),
            pltpu.VMEM((1, grid_z), f32),
            pltpu.VMEM((grid_x, 128), f32),
            pltpu.VMEM((grid_y, 128), f32),
            pltpu.SemaphoreType.DMA((6,)),
            pltpu.SemaphoreType.DMA((part_z // 128 + part_y // SUB - 1,)),
            pltpu.SemaphoreType.DMA,
            pltpu.SemaphoreType.DMA((chunks - 1, per)),
            pltpu.SemaphoreType.DMA((part_z // 128, per)),
            pltpu.SemaphoreType.DMA((chunks - 1, cols - 1)),
            pltpu.SemaphoreType.DMA((3, cols - 1)),
            pltpu.SemaphoreType.DMA((2,)),
            pltpu.SemaphoreType.DMA((max(1, cols // 2 - 1),)),
        ],
        compiler_params=pltpu.CompilerParams(
            collective_id=0, has_side_effects=True, vmem_limit_bytes=47 * 2**20
        ),
    )(velocity, jnp.asarray(held), jnp.asarray(np.ascontiguousarray(t)),
      *(pltpu.with_memory_space_constraint(symbol[None, :], pltpu.HBM) for symbol in (symbol_x, symbol_y, symbol_z)))


def fits(rows, cols, shape):
    grid_x, part_y, part_z = shape
    grid_z = part_z * cols
    held = 7 * grid_x * part_y * part_z * 4 + 4 * grid_z * grid_z + 4 * (grid_x * SUB) ** 2
    even = rows & (rows - 1) == 0 and cols & (cols - 1) == 0 and cols > 1 and grid_x % (16 * rows) == 0
    even = even and grid_x * part_z <= 8 * rows * grid_z
    return even and part_y % SUB == 0 and part_z % 128 == 0 and (part_y * rows) % (SUB * cols) == 0 and held < 54 * 2**20


def local(rows, cols, velocity, symbol_x, symbol_y, symbol_z):
    if fits(rows, cols, velocity.shape):
        return transformed(rows, cols, velocity, symbol_x, symbol_y, symbol_z)
    part_values = along_dim(velocity, 0)
    part_values = lax.all_to_all(part_values, "row", split_axis=0, concat_axis=1, tiled=True)
    pencil_values = along_dim(part_values, 1)
    pencil_values = lax.all_to_all(pencil_values, "col", split_axis=1, concat_axis=2, tiled=True)
    pencil_values = along_dim(pencil_values, 2)
    share_x = pencil_values.shape[0]
    part_x = lax.dynamic_slice_in_dim(symbol_x, lax.axis_index("row") * share_x, share_x)
    share_y = pencil_values.shape[1]
    part_y = lax.dynamic_slice_in_dim(symbol_y, lax.axis_index("col") * share_y, share_y)
    symbol = part_x[:, None, None] + part_y[None, :, None] + symbol_z[None, None, :]
    return pencil_values * ((1.0 - 0.2 * symbol) / (1.0 + 0.2 * symbol))


def solution(mesh):
    placed = (P(None, "row", "col"), P(), P(), P())
    return jax.shard_map(
        functools.partial(local, mesh.shape["row"], mesh.shape["col"]),
        mesh=mesh, in_specs=placed, out_specs=P("row", "col", None), check_vma=False,
    )
```

```python
import functools

import jax
import jax.numpy as jnp
import numpy as np
from jax import lax
from jax.experimental import pallas as pl
from jax.experimental.pallas import tpu as pltpu
from jax.sharding import PartitionSpec as P

SUB = 8
MESH = pl.DeviceIdType.MESH


def mode_table(count):
    rank = jnp.arange(count)
    angle = 2.0 * jnp.pi / count * (rank[:, None] * rank[None, :] % count).astype(jnp.float32)
    return (jnp.cos(angle) + jnp.sin(angle)) * count ** (-0.5)


def along_dim(values, dim):
    moved = jnp.tensordot(
        values, mode_table(values.shape[dim]), axes=([dim], [0]), precision=lax.Precision.HIGHEST
    )
    return jnp.moveaxis(moved, -1, dim)


def fixed_table(count):
    rank = np.arange(count)
    angle = 2.0 * np.pi / count * (rank[:, None] * rank[None, :] % count)
    return ((np.cos(angle) + np.sin(angle)) * count ** (-0.5)).astype(np.float32)


def halves(table):
    high = table.astype(jnp.bfloat16)
    low = (table - high.astype(np.float32)).astype(jnp.bfloat16)
    return high, low


def split(values):
    high = values.astype(jnp.bfloat16)
    low = (values - high.astype(jnp.float32)).astype(jnp.bfloat16)
    return high, low


def product(a, b):
    return jnp.dot(a, b, preferred_element_type=jnp.float32)


def flipped(index, mask):
    out = index
    bit = 1
    while bit <= mask:
        if mask & bit:
            out = out + bit * (1 - 2 * ((index // bit) % 2))
        bit *= 2
    return out


def kernel(
    dims, v_hbm, w_hbm, t_hbm, sx_hbm, sy_hbm, sz_hbm, out_ref,
    v, w, t, v_parts, xs, rbuf, ybuf, zbuf, lhs, factors, raw_in, raw_all, raw_y, sx_row, sy_row, sz_ref, sx_col, sy_col,
    load_sem, v_sem, sent_sem, row_recv, first_recv, col_recv, last_recv, raw_recv, raw_near,
):
    rows, cols, chunks, per, lag, lanes = dims
    part_y, part_z = v.shape[1], v.shape[2]
    grid_x, grid_y = v.shape[0], rbuf.shape[1]
    share_y, grid_z = zbuf.shape[1], zbuf.shape[2]
    tiles, tile = t.shape[1], t.shape[3]
    r, c = lax.axis_index("row"), lax.axis_index("col")
    spans = [pl.ds(p * lanes, lanes) for p in range(part_z // lanes)]

    load_w = pltpu.make_async_copy(w_hbm.at[0], w.at[0], load_sem.at[1])
    load_next = pltpu.make_async_copy(w_hbm.at[1], w.at[1], load_sem.at[6])
    load_rest = pltpu.make_async_copy(w_hbm.at[pl.ds(2, chunks - 2)], w.at[pl.ds(2, chunks - 2)], load_sem.at[2])
    load_t = pltpu.make_async_copy(t_hbm, t, load_sem.at[0])
    groups = [pl.ds(g * SUB, SUB) for g in range(part_y // SUB)]
    parts = [(group, spans[0]) for group in groups] + [(pl.ds(0, part_y), span) for span in spans[1:]]
    load_v = [
        pltpu.make_async_copy(v_hbm.at[:, y, z], v.at[:, y, z], v_sem.at[p]) for p, (y, z) in enumerate(parts)
    ]
    load_symbols = [
        pltpu.make_async_copy(source, target, load_sem.at[3 + n])
        for n, (source, target) in enumerate(((sx_hbm, sx_row), (sy_hbm, sy_row), (sz_hbm, sz_ref)))
    ]
    half = cols // 2
    side = c // half
    row_masks = sorted(range(1, rows), key=lambda m: (-bin(m // 2).count("1"), m))
    row_peers = [flipped(r, m) for m in row_masks]
    near = [flipped(c, m) for m in range(1, half)]
    across = [(half + j) * (1 - side) + (half - 1 - j) * side for j in reversed(range(half))]
    col_peers = near + across
    mirror = cols - 1 - c
    depth = (half - 1 - c) * (1 - side) + (c - half) * side
    marks = list(range(half - 1)) + [2 * half - 2 - depth] * half
    col_targets = list(zip(col_peers, marks))
    raw_widths = [2 * lanes] + [lanes] * (half - 1)

    def by_depth(body):
        for d in range(half):
            pl.when(depth == d)(functools.partial(body, d, raw_widths[d]))

    barrier = pltpu.get_barrier_semaphore()
    for s in row_peers:
        pl.semaphore_signal(barrier, inc=1, device_id=(s, c), device_id_type=MESH)
    for s in col_peers:
        pl.semaphore_signal(barrier, inc=1, device_id=(r, s), device_id_type=MESH)
    load_w.start()
    for load in load_v[:len(groups)]:
        load.start()

    step = SUB * SUB
    whole = pl.ds(0, part_z)
    ends, done = [], 0
    while done < part_z:
        left = part_z - done
        ends.append(pl.ds(done, left // 2 if left % 256 == 0 and len(ends) < 2 else left))
        done += ends[-1].size

    def split_parts(span, picked):
        def part_loop(i, carry):
            for g in picked:
                block = v[pl.ds(i * SUB, SUB), g * SUB:(g + 1) * SUB, span].reshape(step, lanes)
                high, low = split(block)
                v_parts[g, 0, pl.ds(pl.multiple_of(i * step, step), step), span] = high
                v_parts[g, 1, pl.ds(pl.multiple_of(i * step, step), step), span] = low
            return carry

        lax.fori_loop(0, grid_x // SUB, part_loop, 0)

    def x_stage(k, span, picked):
        m, depth = rows * per * SUB, grid_x * SUB
        for g in picked:
            both = product(w[k, :2 * m, :depth], v_parts[g, 0, :, span])
            sums = both[:m] + both[m:] + product(w[k, :m, :depth], v_parts[g, 1, :, span])
            xs[k, :, g * SUB:(g + 1) * SUB, span] = sums.reshape(rows * per, SUB, span.size)

    def own_rows():
        return pl.ds(pl.multiple_of(r * part_y, SUB), part_y)

    def row_stage(k, span, recv):
        for i in range(per):
            for s in row_peers:
                pltpu.make_async_remote_copy(
                    src_ref=xs.at[k, i * rows + s, :, span],
                    dst_ref=rbuf.at[k * per + i, own_rows(), span],
                    send_sem=sent_sem, recv_sem=recv.at[i],
                    device_id=(s, c), device_id_type=MESH,
                ).start()
        for i in range(per):
            rbuf[k * per + i, own_rows(), span] = xs[k, i * rows + r, :, span]

    def y_plane(k, i, span, recv):
        came = rbuf.at[k * per + i, pl.ds(0, grid_y - part_y), span]
        pltpu.make_async_copy(came, came, recv.at[i]).wait()
        high, low = split(rbuf[k * per + i, :, span])
        both = product(w[0, :2 * grid_y, grid_x * SUB:], high)
        ybuf[k, i, :, span] = both[:grid_y] + both[grid_y:] + product(w[0, :grid_y, grid_x * SUB:], low)

    def col_stage(k, i, span, recv, targets):
        at = pl.ds(pl.multiple_of(c * part_z + span.start, 128), span.size)
        for s, mark in targets:
            pltpu.make_async_remote_copy(
                src_ref=ybuf.at[k, i, pl.ds(pl.multiple_of(s * share_y, SUB), share_y), span],
                dst_ref=zbuf.at[k * per + i, :, at],
                send_sem=sent_sem, recv_sem=recv.at[mark],
                device_id=(r, s), device_id_type=MESH,
            ).start()

    def y_stage(k, span, recv):
        for i in range(per):
            y_plane(k, i, span, recv)
            col_stage(k, i, span, col_recv.at[k], col_targets[len(near):] + col_targets[:len(near)])

    def first_y_stage(p):
        span = spans[p]
        for i in range(per):
            y_plane(0, i, span, first_recv.at[p])

            def cross(d, width):
                if i < per - 1 or p * lanes >= width:
                    col_stage(0, i, span, col_recv.at[0], col_targets[len(near):])

            by_depth(cross)
            col_stage(0, i, span, col_recv.at[0], col_targets[:len(near)])

    def raw_stage(p):
        span = spans[p]

        def send(d, width):
            if p * lanes < width:
                pltpu.make_async_remote_copy(
                    src_ref=xs.at[0, pl.ds((per - 1) * rows, rows), :, span], dst_ref=raw_in.at[:, :, span],
                    send_sem=sent_sem, recv_sem=raw_recv.at[0],
                    device_id=(r, mirror), device_id_type=MESH,
                ).start()

        by_depth(send)

    def raw_row_stage(d, width):
        came = raw_in.at[:, :, pl.ds(0, width)]
        pltpu.make_async_copy(came, came, raw_recv.at[0]).wait()
        for s in row_peers:
            pltpu.make_async_remote_copy(
                src_ref=raw_in.at[s, :, pl.ds(0, width)], dst_ref=raw_all.at[own_rows(), pl.ds(0, width)],
                send_sem=sent_sem, recv_sem=raw_recv.at[1],
                device_id=(s, c), device_id_type=MESH,
            ).start()
        raw_all[own_rows(), :width] = raw_in[r, :, :width]

    def raw_y_stage(d, width):
        came = raw_all.at[pl.ds(0, grid_y - part_y), pl.ds(0, width)]
        pltpu.make_async_copy(came, came, raw_recv.at[1]).wait()
        high, low = split(raw_all[:, :width])
        both = product(w[0, :2 * grid_y, grid_x * SUB:], high)
        raw_y[:, :width] = both[:grid_y] + both[grid_y:] + product(w[0, :grid_y, grid_x * SUB:], low)
        at = pl.ds(pl.multiple_of(mirror * part_z, 128), width)
        for m, s in enumerate(near):
            pltpu.make_async_remote_copy(
                src_ref=raw_y.at[pl.ds(pl.multiple_of(s * share_y, SUB), share_y), pl.ds(0, width)],
                dst_ref=zbuf.at[per - 1, :, at],
                send_sem=sent_sem, recv_sem=raw_near.at[m],
                device_id=(r, s), device_id_type=MESH,
            ).start()
        zbuf[per - 1, :, at] = raw_y[pl.ds(pl.multiple_of(c * share_y, SUB), share_y), :width]

    def raw_waits(d, width):
        for m in range(len(near)):
            came = zbuf.at[0, :, pl.ds(0, raw_widths[d ^ (m + 1)])]
            pltpu.make_async_copy(came, came, raw_near.at[m]).wait()

    def last_y_stage(k, recv):
        for i in range(per):
            y_plane(k, i, whole, recv)
        for target in col_targets:
            for q, span in enumerate(ends):
                for i in range(per):
                    col_stage(k, i, span, last_recv.at[q], [target])

    def own_z(k):
        zbuf[pl.ds(k * per, per), :, pl.ds(pl.multiple_of(c * part_z, 128), part_z)] = (
            ybuf[k, :, pl.ds(pl.multiple_of(c * share_y, SUB), share_y), :]
        )

    def col_wait(k, m):
        came = zbuf.at[pl.ds(k * per, per), :, pl.ds(0, part_z)]
        pltpu.make_async_copy(came, came, col_recv.at[k, m]).wait()

    def factor_parts(k, n):
        y_part = sy_col[pl.ds(pl.multiple_of(c * share_y, SUB), share_y), :]
        z_part = sz_ref[:, pl.ds(pl.multiple_of(n * tile, tile), tile)]
        plane = jnp.concatenate([y_part] * (tile // 128), axis=1) + z_part
        for i in range(per):
            x_part = sx_col[pl.ds(r * chunks * per + k * per + i, 1), :]
            symbol = jnp.concatenate([x_part] * (tile // 128), axis=1) + plane
            yield i, (1.0 - 0.2 * symbol) / (1.0 + 0.2 * symbol)

    size = per * share_y

    def scaled(k, n, sums):
        for i, factor in factor_parts(k, n):
            out_ref[k * per + i, :, pl.ds(pl.multiple_of(n * tile, tile), tile)] = (
                sums[i * share_y:(i + 1) * share_y] * factor
            )

    def z_part(k, start, count, finish=None, first=False):
        span = pl.ds(pl.multiple_of(start, 128), count)
        high, low = split(zbuf[pl.ds(k * per, per), :, span].reshape(size, count))
        lhs[:size, :count] = high
        lhs[size:, :count] = low

        def tile_loop(n, carry):
            both = product(lhs[:, :count], t[0, n, span, :])
            sums = both[:size] + both[size:] + product(lhs[:size, :count], t[1, n, span, :])
            at = pl.ds(pl.multiple_of(n * tile, tile), tile)
            if not first:
                sums = sums + out_ref[pl.ds(k * per, per), :, at].reshape(size, tile)
            if finish is None:
                out_ref[pl.ds(k * per, per), :, at] = sums.reshape(per, share_y, tile)
            else:
                finish(k, n, sums)
            return carry

        lax.fori_loop(0, tiles, tile_loop, 0, unroll=8 if count <= 256 else 4)

    def prepare(k):
        def tile_loop(n, carry):
            for i, factor in factor_parts(k, n):
                factors[i, :, pl.ds(pl.multiple_of(n * tile, tile), tile)] = factor
            return carry

        lax.fori_loop(0, tiles, tile_loop, 0)

    def multiplied(k, n, sums):
        at = pl.ds(pl.multiple_of(n * tile, tile), tile)
        out_ref[pl.ds(k * per, per), :, at] = sums.reshape(per, share_y, tile) * factors[:, :, at]

    def last_wait(q, m):
        came = zbuf.at[pl.ds((chunks - 1) * per, per), :, pl.ds(0, ends[q].size)]
        pltpu.make_async_copy(came, came, last_recv.at[q, m]).wait()

    def own_stage(k):
        for m in range(len(near)):
            col_wait(k, m)
        z_part(k, side * half * part_z, half * part_z, first=True)

    def across_stage(k):
        @pl.when(k == 0)
        def _():
            for j in range(half):
                came = zbuf.at[0, :, pl.ds(0, per * part_z - raw_widths[half - 1 - j])]
                pltpu.make_async_copy(came, came, col_recv.at[0, len(near) + j]).wait()
            by_depth(raw_waits)

        @pl.when(k > 0)
        def _():
            for m in range(len(near), len(col_peers)):
                col_wait(k, m)

        z_part(k, (1 - side) * half * part_z, half * part_z, scaled)

    def last_stages():
        before, last = chunks - 2, chunks - 1
        for m in range(len(near)):
            for q in range(len(ends)):
                last_wait(q, m)
        z_part(last, side * half * part_z, half * part_z, first=True)
        prepare(last)
        for j in range(half - 1):
            col_wait(before, len(near) + j)
            z_part(before, across[j] * part_z, part_z)
        for j in range(half - 1):
            for q in range(len(ends)):
                last_wait(q, len(near) + j)
            z_part(last, across[j] * part_z, part_z)
        col_wait(before, len(col_peers) - 1)
        z_part(before, across[-1] * part_z, part_z, scaled)
        for q, span in enumerate(ends):
            last_wait(q, len(col_peers) - 1)
            z_part(last, across[-1] * part_z + span.start, span.size, multiplied if q == len(ends) - 1 else None)

    every = range(len(groups))
    for p, load in enumerate(load_v):
        load.wait()
        if p == 0:
            for later in load_v[len(groups):]:
                later.start()
        if p == len(groups):
            load_next.start()
        n = max(0, p + 1 - len(groups))
        picked = [p] if p < len(groups) else every
        split_parts(spans[n], picked)
        if p == 0:
            load_w.wait()
        x_stage(0, spans[n], picked)
        if p + 1 < len(groups):
            continue
        if n == 0:
            pl.semaphore_wait(barrier, len(row_peers) + len(col_peers))
        row_stage(0, spans[n], first_recv.at[n])
        if n < 2:
            raw_stage(n)
    for load in load_symbols + [load_rest, load_t]:
        load.start()
    load_next.wait()
    x_stage(1, whole, every)
    row_stage(1, whole, row_recv.at[0])
    for p in range(len(spans)):
        first_y_stage(p)
    own_z(0)
    by_depth(raw_row_stage)
    for load in load_symbols:
        load.wait()
    load_rest.wait()
    for ref, column in ((sx_row, sx_col), (sy_row, sy_col)):
        column[...] = jnp.broadcast_to(ref[...], (128, ref.shape[1])).T

    def loop(k, carry):
        @pl.when(k < chunks)
        def _():
            x_stage(k, whole, every)
            row_stage(k, whole, row_recv.at[k - 1])

        @pl.when(k < chunks)
        def _():
            y_stage(k - 1, whole, row_recv.at[k - 2])
            own_z(k - 1)

        @pl.when(k == chunks)
        def _():
            last_y_stage(chunks - 1, row_recv.at[chunks - 2])
            own_z(chunks - 1)

        @pl.when(k == 2)
        def _():
            by_depth(raw_y_stage)
            load_t.wait()

        own_stage(k - lag)

        @pl.when(k >= lag + 1)
        def _():
            across_stage(k - 1 - lag)

        return carry

    lax.fori_loop(2, chunks + lag - 1, loop, 0)
    last_stages()

    def drain(d, width):
        sent = [
            rbuf.at[:, pl.ds(0, grid_y - part_y), :],
            raw_in.at[:, :, pl.ds(0, width)],
            raw_all.at[pl.ds(0, grid_y - part_y), pl.ds(0, width)],
            zbuf.at[pl.ds(1, grid_x // rows - 1), :, pl.ds(0, grid_z - part_z)],
            zbuf.at[0, :, pl.ds(0, grid_z - part_z - half * width)],
        ]
        if near:
            sent.append(raw_y.at[pl.ds(0, len(near) * share_y), pl.ds(0, width)])
        for ref in sent:
            pltpu.make_async_copy(ref, ref, sent_sem).wait()

    by_depth(drain)


def transformed(rows, cols, velocity, symbol_x, symbol_y, symbol_z):
    grid_x, part_y, part_z = velocity.shape
    grid_y, grid_z = part_y * rows, part_z * cols
    share_x, share_y = grid_x // rows, grid_y // cols
    chunks = min(8, share_x)
    per = share_x // chunks
    tile = 256
    hx, hy, hz = fixed_table(grid_x), fixed_table(grid_y), fixed_table(grid_z)
    order = np.arange(grid_x).reshape(rows, chunks, per).transpose(1, 2, 0).reshape(chunks, rows * per)
    w = np.stack([np.kron(hx[o], np.eye(SUB, dtype=np.float32)) for o in order])
    w = np.concatenate(halves(w), axis=1)
    h = np.concatenate(halves(hy), axis=0)
    t = np.stack(halves(hz)).reshape(2, grid_z, grid_z // tile, tile).transpose(0, 2, 1, 3)
    held = np.zeros((chunks, max(w.shape[1], h.shape[0]), w.shape[2] + h.shape[1]), w.dtype)
    held[:, :w.shape[1], :w.shape[2]] = w
    held[0, :h.shape[0], w.shape[2]:] = h
    f32, bf16 = jnp.float32, jnp.bfloat16
    hbm = pl.BlockSpec(memory_space=pltpu.HBM)
    vmem = pl.BlockSpec(memory_space=pltpu.VMEM)
    return pl.pallas_call(
        functools.partial(kernel, (rows, cols, chunks, per, 2, 128)),
        out_shape=jax.ShapeDtypeStruct((share_x, share_y, grid_z), f32),
        in_specs=[hbm] * 6,
        out_specs=vmem,
        scratch_shapes=[
            pltpu.VMEM(velocity.shape, f32),
            pltpu.VMEM(held.shape, bf16),
            pltpu.VMEM(t.shape, bf16),
            pltpu.VMEM((part_y // SUB, 2, grid_x * SUB, part_z), bf16),
            pltpu.VMEM((chunks, rows * per, part_y, part_z), f32),
            pltpu.VMEM((share_x, grid_y, part_z), f32),
            pltpu.VMEM((chunks, per, grid_y, part_z), f32),
            pltpu.VMEM((share_x, share_y, grid_z), f32),
            pltpu.VMEM((2 * per * share_y, grid_z), bf16),
            pltpu.VMEM((per, share_y, grid_z), f32),
            pltpu.VMEM((rows, part_y, 2 * 128), f32),
            pltpu.VMEM((grid_y, 2 * 128), f32),
            pltpu.VMEM((grid_y, 2 * 128), f32),
            pltpu.VMEM((1, grid_x), f32),
            pltpu.VMEM((1, grid_y), f32),
            pltpu.VMEM((1, grid_z), f32),
            pltpu.VMEM((grid_x, 128), f32),
            pltpu.VMEM((grid_y, 128), f32),
            pltpu.SemaphoreType.DMA((7,)),
            pltpu.SemaphoreType.DMA((part_z // 128 + part_y // SUB - 1,)),
            pltpu.SemaphoreType.DMA,
            pltpu.SemaphoreType.DMA((chunks - 1, per)),
            pltpu.SemaphoreType.DMA((part_z // 128, per)),
            pltpu.SemaphoreType.DMA((chunks - 1, cols - 1)),
            pltpu.SemaphoreType.DMA((3, cols - 1)),
            pltpu.SemaphoreType.DMA((2,)),
            pltpu.SemaphoreType.DMA((max(1, cols // 2 - 1),)),
        ],
        compiler_params=pltpu.CompilerParams(
            collective_id=0, has_side_effects=True, vmem_limit_bytes=47 * 2**20
        ),
    )(velocity, jnp.asarray(held), jnp.asarray(np.ascontiguousarray(t)),
      *(pltpu.with_memory_space_constraint(symbol[None, :], pltpu.HBM) for symbol in (symbol_x, symbol_y, symbol_z)))


def fits(rows, cols, shape):
    grid_x, part_y, part_z = shape
    grid_z = part_z * cols
    held = 7 * grid_x * part_y * part_z * 4 + 4 * grid_z * grid_z + 4 * (grid_x * SUB) ** 2
    even = rows & (rows - 1) == 0 and cols & (cols - 1) == 0 and cols > 1 and grid_x % (16 * rows) == 0
    even = even and grid_x * part_z <= 8 * rows * grid_z
    return even and part_y % SUB == 0 and part_z % 256 == 0 and (part_y * rows) % (SUB * cols) == 0 and held < 54 * 2**20


def local(rows, cols, velocity, symbol_x, symbol_y, symbol_z):
    if fits(rows, cols, velocity.shape):
        return transformed(rows, cols, velocity, symbol_x, symbol_y, symbol_z)
    part_values = along_dim(velocity, 0)
    part_values = lax.all_to_all(part_values, "row", split_axis=0, concat_axis=1, tiled=True)
    pencil_values = along_dim(part_values, 1)
    pencil_values = lax.all_to_all(pencil_values, "col", split_axis=1, concat_axis=2, tiled=True)
    pencil_values = along_dim(pencil_values, 2)
    share_x = pencil_values.shape[0]
    part_x = lax.dynamic_slice_in_dim(symbol_x, lax.axis_index("row") * share_x, share_x)
    share_y = pencil_values.shape[1]
    part_y = lax.dynamic_slice_in_dim(symbol_y, lax.axis_index("col") * share_y, share_y)
    symbol = part_x[:, None, None] + part_y[None, :, None] + symbol_z[None, None, :]
    return pencil_values * ((1.0 - 0.2 * symbol) / (1.0 + 0.2 * symbol))


def solution(mesh):
    placed = (P(None, "row", "col"), P(), P(), P())
    return jax.shard_map(
        functools.partial(local, mesh.shape["row"], mesh.shape["col"]),
        mesh=mesh, in_specs=placed, out_specs=P("row", "col", None), check_vma=False,
    )
```

```python
import functools

import jax
import jax.numpy as jnp
import numpy as np
from jax import lax
from jax.experimental import pallas as pl
from jax.experimental.pallas import tpu as pltpu
from jax.sharding import PartitionSpec as P

SUB = 8
MESH = pl.DeviceIdType.MESH


def mode_table(count):
    rank = jnp.arange(count)
    angle = 2.0 * jnp.pi / count * (rank[:, None] * rank[None, :] % count).astype(jnp.float32)
    return (jnp.cos(angle) + jnp.sin(angle)) * count ** (-0.5)


def along_dim(values, dim):
    moved = jnp.tensordot(
        values, mode_table(values.shape[dim]), axes=([dim], [0]), precision=lax.Precision.HIGHEST
    )
    return jnp.moveaxis(moved, -1, dim)


def fixed_table(count):
    rank = np.arange(count)
    angle = 2.0 * np.pi / count * (rank[:, None] * rank[None, :] % count)
    return ((np.cos(angle) + np.sin(angle)) * count ** (-0.5)).astype(np.float32)


def halves(table):
    high = table.astype(jnp.bfloat16)
    low = (table - high.astype(np.float32)).astype(jnp.bfloat16)
    return high, low


def split(values):
    high = values.astype(jnp.bfloat16)
    low = (values - high.astype(jnp.float32)).astype(jnp.bfloat16)
    return high, low


def product(a, b):
    return jnp.dot(a, b, preferred_element_type=jnp.float32)


def flipped(index, mask):
    out = index
    bit = 1
    while bit <= mask:
        if mask & bit:
            out = out + bit * (1 - 2 * ((index // bit) % 2))
        bit *= 2
    return out


def kernel(
    dims, v_hbm, w_hbm, t_hbm, sx_hbm, sy_hbm, sz_hbm, out_ref,
    v, w, t, v_parts, xs, rbuf, ybuf, zbuf, lhs, factors, raw_in, raw_all, raw_y, sx_row, sy_row, sz_ref, sx_col, sy_col,
    load_sem, v_sem, sent_sem, row_recv, first_recv, col_recv, last_recv, raw_recv, raw_near,
):
    rows, cols, chunks, per, lag, lanes = dims
    part_y, part_z = v.shape[1], v.shape[2]
    grid_x, grid_y = v.shape[0], rbuf.shape[1]
    share_y, grid_z = zbuf.shape[1], zbuf.shape[2]
    tiles, tile = t.shape[1], t.shape[3]
    r, c = lax.axis_index("row"), lax.axis_index("col")
    spans = [pl.ds(p * lanes, lanes) for p in range(part_z // lanes)]

    load_w = pltpu.make_async_copy(w_hbm.at[0], w.at[0], load_sem.at[1])
    load_next = pltpu.make_async_copy(w_hbm.at[1], w.at[1], load_sem.at[4])
    load_rest = pltpu.make_async_copy(w_hbm.at[pl.ds(2, chunks - 2)], w.at[pl.ds(2, chunks - 2)], load_sem.at[2])
    load_t = pltpu.make_async_copy(t_hbm, t, load_sem.at[0])
    groups = [pl.ds(g * SUB, SUB) for g in range(part_y // SUB)]
    parts = [(group, spans[0]) for group in groups] + [(pl.ds(0, part_y), span) for span in spans[1:]]
    load_v = [
        pltpu.make_async_copy(v_hbm.at[:, y, z], v.at[:, y, z], v_sem.at[p]) for p, (y, z) in enumerate(parts)
    ]
    load_symbols = [
        pltpu.make_async_copy(source, target, load_sem.at[3])
        for source, target in ((sx_hbm, sx_row), (sy_hbm, sy_row), (sz_hbm, sz_ref))
    ]
    half = cols // 2
    side = c // half
    row_masks = sorted(range(1, rows), key=lambda m: (-bin(m // 2).count("1"), m))
    row_peers = [flipped(r, m) for m in row_masks]
    near = [flipped(c, m) for m in range(1, half)]
    across = [(half + j) * (1 - side) + (half - 1 - j) * side for j in reversed(range(half))]
    col_peers = near + across
    mirror = cols - 1 - c
    depth = (half - 1 - c) * (1 - side) + (c - half) * side
    marks = list(range(half - 1)) + [2 * half - 2 - depth] * half
    col_targets = list(zip(col_peers, marks))
    raw_widths = [2 * lanes] + [lanes] * (half - 1)

    def by_depth(body):
        for d in range(half):
            pl.when(depth == d)(functools.partial(body, d, raw_widths[d]))

    barrier = pltpu.get_barrier_semaphore()
    for s in row_peers:
        pl.semaphore_signal(barrier, inc=1, device_id=(s, c), device_id_type=MESH)
    for s in col_peers:
        pl.semaphore_signal(barrier, inc=1, device_id=(r, s), device_id_type=MESH)
    load_w.start()
    for load in load_v[:len(groups)]:
        load.start()

    step = SUB * SUB
    whole = pl.ds(0, part_z)
    ends, done = [], 0
    while done < part_z:
        left = part_z - done
        ends.append(pl.ds(done, left // 2 if left % 256 == 0 and len(ends) < 2 else left))
        done += ends[-1].size

    def split_parts(span, picked):
        def part_loop(i, carry):
            for g in picked:
                block = v[pl.ds(i * SUB, SUB), g * SUB:(g + 1) * SUB, span].reshape(step, lanes)
                high, low = split(block)
                v_parts[g, 0, pl.ds(pl.multiple_of(i * step, step), step), span] = high
                v_parts[g, 1, pl.ds(pl.multiple_of(i * step, step), step), span] = low
            return carry

        lax.fori_loop(0, grid_x // SUB, part_loop, 0)

    def x_stage(k, span, picked):
        m, depth = rows * per * SUB, grid_x * SUB
        for g in picked:
            both = product(w[k, :2 * m, :depth], v_parts[g, 0, :, span])
            sums = both[:m] + both[m:] + product(w[k, :m, :depth], v_parts[g, 1, :, span])
            xs[k, :, g * SUB:(g + 1) * SUB, span] = sums.reshape(rows * per, SUB, span.size)

    def own_rows():
        return pl.ds(pl.multiple_of(r * part_y, SUB), part_y)

    def row_stage(k, span, recv):
        for i in range(per):
            for s in row_peers:
                pltpu.make_async_remote_copy(
                    src_ref=xs.at[k, i * rows + s, :, span],
                    dst_ref=rbuf.at[k * per + i, own_rows(), span],
                    send_sem=sent_sem, recv_sem=recv.at[i],
                    device_id=(s, c), device_id_type=MESH,
                ).start()
        for i in range(per):
            rbuf[k * per + i, own_rows(), span] = xs[k, i * rows + r, :, span]

    def y_plane(k, i, span, recv):
        came = rbuf.at[k * per + i, pl.ds(0, grid_y - part_y), span]
        pltpu.make_async_copy(came, came, recv.at[i]).wait()
        high, low = split(rbuf[k * per + i, :, span])
        both = product(w[0, :2 * grid_y, grid_x * SUB:], high)
        ybuf[k, i, :, span] = both[:grid_y] + both[grid_y:] + product(w[0, :grid_y, grid_x * SUB:], low)

    def col_at(k, mark):
        if isinstance(mark, int) and mark < len(near):
            return k * half + mark
        return k * half + len(near) + (mark - len(near)) * (k // (chunks - 2))

    def col_stage(k, i, span, recv, targets):
        at = pl.ds(pl.multiple_of(c * part_z + span.start, 128), span.size)
        for s, mark in targets:
            pltpu.make_async_remote_copy(
                src_ref=ybuf.at[k, i, pl.ds(pl.multiple_of(s * share_y, SUB), share_y), span],
                dst_ref=zbuf.at[k * per + i, :, at],
                send_sem=sent_sem, recv_sem=col_recv.at[col_at(k, mark)] if recv is None else recv.at[mark],
                device_id=(r, s), device_id_type=MESH,
            ).start()

    def y_stage(k, span, recv):
        for i in range(per):
            y_plane(k, i, span, recv)
            col_stage(k, i, span, None, col_targets[len(near):] + col_targets[:len(near)])

    def first_y_stage(p):
        span = spans[p]
        for i in range(per):
            y_plane(0, i, span, first_recv.at[p])

            def cross(d, width):
                if i < per - 1 or p * lanes >= width:
                    col_stage(0, i, span, None, col_targets[len(near):])

            by_depth(cross)
            col_stage(0, i, span, None, col_targets[:len(near)])

    def raw_stage(p):
        span = spans[p]

        def send(d, width):
            if p * lanes < width:
                pltpu.make_async_remote_copy(
                    src_ref=xs.at[0, pl.ds((per - 1) * rows, rows), :, span], dst_ref=raw_in.at[:, :, span],
                    send_sem=sent_sem, recv_sem=raw_recv.at[0],
                    device_id=(r, mirror), device_id_type=MESH,
                ).start()

        by_depth(send)

    def raw_row_stage(d, width):
        came = raw_in.at[:, :, pl.ds(0, width)]
        pltpu.make_async_copy(came, came, raw_recv.at[0]).wait()
        for s in row_peers:
            pltpu.make_async_remote_copy(
                src_ref=raw_in.at[s, :, pl.ds(0, width)], dst_ref=raw_all.at[own_rows(), pl.ds(0, width)],
                send_sem=sent_sem, recv_sem=raw_recv.at[1],
                device_id=(s, c), device_id_type=MESH,
            ).start()
        raw_all[own_rows(), :width] = raw_in[r, :, :width]

    def raw_y_stage(d, width):
        came = raw_all.at[pl.ds(0, grid_y - part_y), pl.ds(0, width)]
        pltpu.make_async_copy(came, came, raw_recv.at[1]).wait()
        high, low = split(raw_all[:, :width])
        both = product(w[0, :2 * grid_y, grid_x * SUB:], high)
        raw_y[:, :width] = both[:grid_y] + both[grid_y:] + product(w[0, :grid_y, grid_x * SUB:], low)
        at = pl.ds(pl.multiple_of(mirror * part_z, 128), width)
        for m, s in enumerate(near):
            pltpu.make_async_remote_copy(
                src_ref=raw_y.at[pl.ds(pl.multiple_of(s * share_y, SUB), share_y), pl.ds(0, width)],
                dst_ref=zbuf.at[per - 1, :, at],
                send_sem=sent_sem, recv_sem=raw_near.at[m],
                device_id=(r, s), device_id_type=MESH,
            ).start()
        zbuf[per - 1, :, at] = raw_y[pl.ds(pl.multiple_of(c * share_y, SUB), share_y), :width]

    def raw_waits(d, width):
        for m in range(len(near)):
            came = zbuf.at[0, :, pl.ds(0, raw_widths[d ^ (m + 1)])]
            pltpu.make_async_copy(came, came, raw_near.at[m]).wait()

    def last_y_stage(k, recv):
        for i in range(per):
            y_plane(k, i, whole, recv)
        for target in col_targets:
            for q, span in enumerate(ends):
                for i in range(per):
                    col_stage(k, i, span, last_recv.at[q], [target])

    def own_z(k):
        zbuf[pl.ds(k * per, per), :, pl.ds(pl.multiple_of(c * part_z, 128), part_z)] = (
            ybuf[k, :, pl.ds(pl.multiple_of(c * share_y, SUB), share_y), :]
        )

    def col_wait(k, m):
        came = zbuf.at[pl.ds(k * per, per), :, pl.ds(0, part_z)]
        pltpu.make_async_copy(came, came, col_recv.at[col_at(k, m)]).wait()

    def factor_parts(k, n):
        y_part = sy_col[pl.ds(pl.multiple_of(c * share_y, SUB), share_y), :]
        z_part = sz_ref[:, pl.ds(pl.multiple_of(n * tile, tile), tile)]
        plane = jnp.concatenate([y_part] * (tile // 128), axis=1) + z_part
        for i in range(per):
            x_part = sx_col[pl.ds(r * chunks * per + k * per + i, 1), :]
            symbol = jnp.concatenate([x_part] * (tile // 128), axis=1) + plane
            yield i, (1.0 - 0.2 * symbol) / (1.0 + 0.2 * symbol)

    size = per * share_y

    def scaled(k, n, sums):
        for i, factor in factor_parts(k, n):
            out_ref[k * per + i, :, pl.ds(pl.multiple_of(n * tile, tile), tile)] = (
                sums[i * share_y:(i + 1) * share_y] * factor
            )

    def z_part(k, start, count, finish=None, first=False):
        span = pl.ds(pl.multiple_of(start, 128), count)
        high, low = split(zbuf[pl.ds(k * per, per), :, span].reshape(size, count))
        lhs[:size, :count] = high
        lhs[size:, :count] = low

        def tile_loop(n, carry):
            both = product(lhs[:, :count], t[0, n, span, :])
            sums = both[:size] + both[size:] + product(lhs[:size, :count], t[1, n, span, :])
            at = pl.ds(pl.multiple_of(n * tile, tile), tile)
            if not first:
                sums = sums + out_ref[pl.ds(k * per, per), :, at].reshape(size, tile)
            if finish is None:
                out_ref[pl.ds(k * per, per), :, at] = sums.reshape(per, share_y, tile)
            else:
                finish(k, n, sums)
            return carry

        lax.fori_loop(0, tiles, tile_loop, 0, unroll=8 if count <= 256 else 4)

    def prepare(k):
        def tile_loop(n, carry):
            for i, factor in factor_parts(k, n):
                factors[i, :, pl.ds(pl.multiple_of(n * tile, tile), tile)] = factor
            return carry

        lax.fori_loop(0, tiles, tile_loop, 0)

    def multiplied(k, n, sums):
        at = pl.ds(pl.multiple_of(n * tile, tile), tile)
        out_ref[pl.ds(k * per, per), :, at] = sums.reshape(per, share_y, tile) * factors[:, :, at]

    def last_wait(q, m):
        came = zbuf.at[pl.ds((chunks - 1) * per, per), :, pl.ds(0, ends[q].size)]
        pltpu.make_async_copy(came, came, last_recv.at[q, m]).wait()

    def own_stage(k):
        for m in range(len(near)):
            col_wait(k, m)
        z_part(k, side * half * part_z, half * part_z, first=True)

    def across_stage(k):
        @pl.when(k == 0)
        def _():
            came = zbuf.at[0, :, pl.ds(0, half * per * part_z - sum(raw_widths))]
            pltpu.make_async_copy(came, came, col_recv.at[len(near)]).wait()
            by_depth(raw_waits)

        @pl.when(k > 0)
        def _():
            came = zbuf.at[pl.ds(k * per, per), :, pl.ds(0, half * part_z)]
            pltpu.make_async_copy(came, came, col_recv.at[col_at(k, len(near))]).wait()

        z_part(k, (1 - side) * half * part_z, half * part_z, scaled)

    def last_stages():
        before, last = chunks - 2, chunks - 1
        for m in range(len(near)):
            for q in range(len(ends)):
                last_wait(q, m)
        z_part(last, side * half * part_z, half * part_z, first=True)
        prepare(last)
        for j in range(half - 1):
            col_wait(before, len(near) + j)
            z_part(before, across[j] * part_z, part_z)
        for j in range(half - 1):
            for q in range(len(ends)):
                last_wait(q, len(near) + j)
            z_part(last, across[j] * part_z, part_z)
        col_wait(before, len(col_peers) - 1)
        z_part(before, across[-1] * part_z, part_z, scaled)
        for q, span in enumerate(ends):
            last_wait(q, len(col_peers) - 1)
            z_part(last, across[-1] * part_z + span.start, span.size, multiplied if q == len(ends) - 1 else None)

    every = range(len(groups))
    for p, load in enumerate(load_v):
        load.wait()
        if p == 0:
            for later in load_v[len(groups):]:
                later.start()
        if p == len(groups):
            load_next.start()
        n = max(0, p + 1 - len(groups))
        picked = [p] if p < len(groups) else every
        split_parts(spans[n], picked)
        if p == 0:
            load_w.wait()
        x_stage(0, spans[n], picked)
        if p + 1 < len(groups):
            continue
        if n == 0:
            pl.semaphore_wait(barrier, len(row_peers) + len(col_peers))
        row_stage(0, spans[n], first_recv.at[n])
        if n < 2:
            raw_stage(n)
    for load in load_symbols + [load_rest, load_t]:
        load.start()
    load_next.wait()
    x_stage(1, whole, every)
    row_stage(1, whole, row_recv.at[0])
    for p in range(len(spans)):
        first_y_stage(p)
    own_z(0)
    by_depth(raw_row_stage)
    for load in load_symbols:
        load.wait()
    load_rest.wait()
    for ref, column in ((sx_row, sx_col), (sy_row, sy_col)):
        column[...] = jnp.broadcast_to(ref[...], (128, ref.shape[1])).T

    def loop(k, carry):
        @pl.when(k < chunks)
        def _():
            x_stage(k, whole, every)
            row_stage(k, whole, row_recv.at[k - 1])

        @pl.when(k < chunks)
        def _():
            y_stage(k - 1, whole, row_recv.at[k - 2])
            own_z(k - 1)

        @pl.when(k == chunks)
        def _():
            last_y_stage(chunks - 1, row_recv.at[chunks - 2])
            own_z(chunks - 1)

        @pl.when(k == 2)
        def _():
            by_depth(raw_y_stage)
            load_t.wait()

        own_stage(k - lag)

        @pl.when(k >= lag + 1)
        def _():
            across_stage(k - 1 - lag)

        return carry

    lax.fori_loop(2, chunks + lag - 1, loop, 0)
    last_stages()

    def drain(d, width):
        sent = [
            rbuf.at[:, pl.ds(0, grid_y - part_y), :],
            raw_in.at[:, :, pl.ds(0, width)],
            raw_all.at[pl.ds(0, grid_y - part_y), pl.ds(0, width)],
            zbuf.at[pl.ds(1, grid_x // rows - 1), :, pl.ds(0, grid_z - part_z)],
            zbuf.at[0, :, pl.ds(0, grid_z - part_z - half * width)],
        ]
        if near:
            sent.append(raw_y.at[pl.ds(0, len(near) * share_y), pl.ds(0, width)])
        for ref in sent:
            pltpu.make_async_copy(ref, ref, sent_sem).wait()

    by_depth(drain)


def transformed(rows, cols, velocity, symbol_x, symbol_y, symbol_z):
    grid_x, part_y, part_z = velocity.shape
    grid_y, grid_z = part_y * rows, part_z * cols
    share_x, share_y = grid_x // rows, grid_y // cols
    chunks = min(8, share_x)
    per = share_x // chunks
    tile = 256
    hx, hy, hz = fixed_table(grid_x), fixed_table(grid_y), fixed_table(grid_z)
    order = np.arange(grid_x).reshape(rows, chunks, per).transpose(1, 2, 0).reshape(chunks, rows * per)
    w = np.stack([np.kron(hx[o], np.eye(SUB, dtype=np.float32)) for o in order])
    w = np.concatenate(halves(w), axis=1)
    h = np.concatenate(halves(hy), axis=0)
    t = np.stack(halves(hz)).reshape(2, grid_z, grid_z // tile, tile).transpose(0, 2, 1, 3)
    held = np.zeros((chunks, max(w.shape[1], h.shape[0]), w.shape[2] + h.shape[1]), w.dtype)
    held[:, :w.shape[1], :w.shape[2]] = w
    held[0, :h.shape[0], w.shape[2]:] = h
    f32, bf16 = jnp.float32, jnp.bfloat16
    hbm = pl.BlockSpec(memory_space=pltpu.HBM)
    vmem = pl.BlockSpec(memory_space=pltpu.VMEM)
    return pl.pallas_call(
        functools.partial(kernel, (rows, cols, chunks, per, 2, 128)),
        out_shape=jax.ShapeDtypeStruct((share_x, share_y, grid_z), f32),
        in_specs=[hbm] * 6,
        out_specs=vmem,
        scratch_shapes=[
            pltpu.VMEM(velocity.shape, f32),
            pltpu.VMEM(held.shape, bf16),
            pltpu.VMEM(t.shape, bf16),
            pltpu.VMEM((part_y // SUB, 2, grid_x * SUB, part_z), bf16),
            pltpu.VMEM((chunks, rows * per, part_y, part_z), f32),
            pltpu.VMEM((share_x, grid_y, part_z), f32),
            pltpu.VMEM((chunks, per, grid_y, part_z), f32),
            pltpu.VMEM((share_x, share_y, grid_z), f32),
            pltpu.VMEM((2 * per * share_y, grid_z), bf16),
            pltpu.VMEM((per, share_y, grid_z), f32),
            pltpu.VMEM((rows, part_y, 2 * 128), f32),
            pltpu.VMEM((grid_y, 2 * 128), f32),
            pltpu.VMEM((grid_y, 2 * 128), f32),
            pltpu.VMEM((1, grid_x), f32),
            pltpu.VMEM((1, grid_y), f32),
            pltpu.VMEM((1, grid_z), f32),
            pltpu.VMEM((grid_x, 128), f32),
            pltpu.VMEM((grid_y, 128), f32),
            pltpu.SemaphoreType.DMA((5,)),
            pltpu.SemaphoreType.DMA((part_z // 128 + part_y // SUB - 1,)),
            pltpu.SemaphoreType.DMA,
            pltpu.SemaphoreType.DMA((chunks - 1, per)),
            pltpu.SemaphoreType.DMA((part_z // 128, per)),
            pltpu.SemaphoreType.DMA(((chunks - 1) * (cols // 2) + cols // 2 - 1,)),
            pltpu.SemaphoreType.DMA((3, cols - 1)),
            pltpu.SemaphoreType.DMA((2,)),
            pltpu.SemaphoreType.DMA((max(1, cols // 2 - 1),)),
        ],
        compiler_params=pltpu.CompilerParams(
            collective_id=0, has_side_effects=True, vmem_limit_bytes=47 * 2**20
        ),
    )(velocity, jnp.asarray(held), jnp.asarray(np.ascontiguousarray(t)),
      *(pltpu.with_memory_space_constraint(symbol[None, :], pltpu.HBM) for symbol in (symbol_x, symbol_y, symbol_z)))


def fits(rows, cols, shape):
    grid_x, part_y, part_z = shape
    grid_z = part_z * cols
    held = 7 * grid_x * part_y * part_z * 4 + 4 * grid_z * grid_z + 4 * (grid_x * SUB) ** 2
    even = rows & (rows - 1) == 0 and cols & (cols - 1) == 0 and cols > 1 and grid_x % (16 * rows) == 0
    even = even and grid_x * part_z * (cols // 2) <= 8 * rows * grid_z
    return even and part_y % SUB == 0 and part_z % 256 == 0 and (part_y * rows) % (SUB * cols) == 0 and held < 54 * 2**20


def local(rows, cols, velocity, symbol_x, symbol_y, symbol_z):
    if fits(rows, cols, velocity.shape):
        return transformed(rows, cols, velocity, symbol_x, symbol_y, symbol_z)
    part_values = along_dim(velocity, 0)
    part_values = lax.all_to_all(part_values, "row", split_axis=0, concat_axis=1, tiled=True)
    pencil_values = along_dim(part_values, 1)
    pencil_values = lax.all_to_all(pencil_values, "col", split_axis=1, concat_axis=2, tiled=True)
    pencil_values = along_dim(pencil_values, 2)
    share_x = pencil_values.shape[0]
    part_x = lax.dynamic_slice_in_dim(symbol_x, lax.axis_index("row") * share_x, share_x)
    share_y = pencil_values.shape[1]
    part_y = lax.dynamic_slice_in_dim(symbol_y, lax.axis_index("col") * share_y, share_y)
    symbol = part_x[:, None, None] + part_y[None, :, None] + symbol_z[None, None, :]
    return pencil_values * ((1.0 - 0.2 * symbol) / (1.0 + 0.2 * symbol))


def solution(mesh):
    placed = (P(None, "row", "col"), P(), P(), P())
    return jax.shard_map(
        functools.partial(local, mesh.shape["row"], mesh.shape["col"]),
        mesh=mesh, in_specs=placed, out_specs=P("row", "col", None), check_vma=False,
    )
```
